768 devices in a mesh: section: 16 (over y, core), tensor: 4 (over z_lo), dp: 12 (over z_hi, x).
Axes of the slice: x: 4, y: 8, z: 12 (z_hi: 3, z_lo: 4; z = z_hi * 4 + z_lo), core: 2. Of those that a mesh axis runs over, the one named last changes fastest.
Arguments:
- acts: bfloat16 [16, 24, 256, 2048], P('section', 'dp', 'tensor'), parts along dimension 1, may hold values from -6 to 6
- fresh: bfloat16 [24, 256, 2048], P('dp', 'tensor'), parts along dimension 0, may hold values from -6 to 6
- order: int32 [16, 2], P('section'), may hold values from 0 to 1
- ln_gain: float32 [16, 2048], P('section'), may hold values from 0.1 to 1.9
- ln_bias: float32 [16, 2048], P('section'), may hold values from -3 to 3
- wqkv: bfloat16 [16, 2048, 6144], P('section', None, 'tensor'), may hold values from -4 to 4
- wo: bfloat16 [16, 2048, 2048], P('section', 'tensor'), may hold values from -0.125 to 0.125
Outputs:
- section_out: bfloat16 [24, 16, 256, 2048], P('dp', 'section', 'tensor'), parts along dimension 0
- held: bfloat16 [16, 24, 256, 2048], P('section', 'dp', 'tensor'), parts along dimension 1
The draws below stay inside these ranges and needn't reach their ends.
There are 12 independent parts, one for each index of `dp`. The reference program is written for one: setup_inputs(seed, part) draws one part's arguments, and reference() takes and returns one part's arrays. A program takes and returns all parts, laid end to end along the dimension named above; an argument that names none is the same for every part. Nothing has to cross between parts.
All inputs are finite; a program needn't handle non-finite values.
Results may differ from the reference program's by a relative error of at most 0.017.
Values may be sent and summed in bfloat16 or wider, within the bound.
A program may use at most 64 MiB of HBM per device.

```python
import jax
import jax.numpy as jnp
from jax import lax

D = 2048
HEADS = 16
HD = 128
SEQ = 256
SLOTS = 2
TICKS = 2
SECTIONS = 16
N_TENSOR = 4


def draw_wqkv(key, part):
    first = jax.random.fold_in(jax.random.fold_in(key, 11), 0)
    base = jnp.clip(jax.random.normal(first, (SECTIONS, D, HEADS, 3, HD), jnp.float32), -6.0, 6.0) * D ** (-0.5)
    return base.reshape(SECTIONS, D, HEADS * 3 * HD).astype(jnp.bfloat16)


def with_ends(values, own_key, smallest, largest):
    longest = values.shape.index(max(values.shape))
    spots = []
    for shift in (0, 1):
        where = [jax.random.randint(jax.random.fold_in(own_key, axis), (), 0, length) for axis, length in enumerate(values.shape)]
        where[longest] = (where[longest] + shift) % values.shape[longest]
        spots.append(tuple(where))
    return values.at[spots[0]].set(smallest).at[spots[1]].set(largest)


def level_of(rng, shape, cuts, low, high):
    loudness = 1.0
    for axis_at, blocks in cuts:
        steps = jax.random.uniform(jax.random.fold_in(jax.random.fold_in(rng, 6), axis_at), (blocks,), jnp.float32, low / len(cuts), high / len(cuts))
        loudness = loudness * jnp.repeat(jnp.exp(steps), shape[axis_at] // blocks).reshape((-1,) + (1,) * (len(shape) - 1 - axis_at))
    return loudness


def normal_values(rng, shape, scale, limit, cuts=(), kind=jnp.bfloat16):
    entries = jax.random.normal(rng, shape, jnp.float32) * scale
    if len(cuts) > 0:
        entries = level_of(rng, shape, cuts, -0.22, 0.18) * entries
    return jnp.clip(entries, min=-limit, max=limit).astype(kind)


def setup_inputs(seed: int = 0, part: int = 0) -> dict:
    key_list = jax.random.split(jax.random.key(seed), 8)
    own_keys = jax.random.split(jax.random.fold_in(key_list[7], part), 8)
    acts = normal_values(own_keys[0], (SECTIONS, SLOTS, SEQ, D), 1.0, 6.0, ((0, 16), (2, 4)))
    fresh = normal_values(own_keys[1], (TICKS, SEQ, D), 1.0, 6.0, ((1, 4),))
    order = with_ends(jax.random.randint(key_list[2], (SECTIONS, TICKS), 0, SLOTS), jax.random.fold_in(key_list[2], 1), 0, SLOTS - 1).astype(jnp.int32)
    ln_gain = jnp.clip(1.0 + 0.18 * jax.random.normal(key_list[3], (SECTIONS, D), jnp.float32), 0.1, 1.9)
    ln_bias = normal_values(key_list[4], (SECTIONS, D), 0.5, 3.0, ((0, 16),), jnp.float32)
    wqkv = draw_wqkv(jax.random.fold_in(key_list[7], 71), part)
    wo = normal_values(key_list[6], (SECTIONS, HEADS * HD, D), (HEADS * HD) ** -0.5, 0.125, ((0, 16), (1, 4)))
    return {"acts": acts, "fresh": fresh, "order": order, "ln_gain": ln_gain, "ln_bias": ln_bias, "wqkv": wqkv, "wo": wo}


def normed(rows, gain, bias):
    values = rows.astype(jnp.float32)
    centred = values - lax.optimization_barrier(jnp.mean(values, axis=-1, keepdims=True))
    spread = lax.optimization_barrier(jnp.mean(centred * centred, axis=-1, keepdims=True))
    return (centred * lax.rsqrt(spread + 1e-06) * gain + bias).astype(jnp.bfloat16)

def layer(inputs):
    rows, gain, bias, w_in, w_out = inputs
    normal_rows = normed(rows, gain, bias)
    qkv = jnp.dot(normal_rows, w_in, preferred_element_type=jnp.float32).astype(jnp.bfloat16)
    grid = qkv.reshape(SEQ, HEADS, 3, HD).astype(jnp.float32)
    scores = jnp.einsum('qhe,khe->hqk', grid[:, :, 0], grid[:, :, 1]) / jnp.sqrt(jnp.float32(HD))
    probs = jax.nn.softmax(scores, axis=-1).astype(jnp.bfloat16)
    attn = jnp.einsum('hqk,khe->qhe', probs.astype(jnp.float32), grid[:, :, 2]).astype(jnp.bfloat16)
    grouped = attn.reshape(SEQ, N_TENSOR, HEADS // N_TENSOR * HD).astype(jnp.float32)
    wo_grouped = w_out.reshape(N_TENSOR, HEADS // N_TENSOR * HD, D).astype(jnp.float32)
    partial_value = jnp.einsum('sgc,gcd->gsd', grouped, wo_grouped).astype(jnp.bfloat16)
    partial_value = lax.optimization_barrier(partial_value)
    total = lax.optimization_barrier(jnp.sum(partial_value.astype(jnp.float32), axis=0))
    return (rows.astype(jnp.float32) + total).astype(jnp.bfloat16)

def reference(acts, fresh, order, ln_gain, ln_bias, wqkv, wo):
    slots = acts
    outputs = []
    slot_ids = jnp.arange(SLOTS, dtype=jnp.int32)
    for tick in range(TICKS):
        chosen = order[:, tick].astype(jnp.int32)
        picked = jnp.take_along_axis(slots, chosen[:, None, None, None], axis=1)[:, 0]
        results = lax.map(layer, (picked, ln_gain, ln_bias, wqkv, wo))
        outputs.append(results)
        incoming = jnp.concatenate([fresh[tick][None], results[:-1]], axis=0)
        marks = (slot_ids[None, :] == chosen[:, None])[:, :, None, None]
        slots = jnp.where(marks, incoming[:, None], slots)
    return (jnp.stack(outputs, axis=0), slots)
```

```python
import functools
import math

import jax
import jax.numpy as jnp
from jax import lax
from jax.experimental import pallas as pl
from jax.experimental.pallas import tpu as pltpu
from jax.sharding import PartitionSpec as P

HD = 128
TICKS = 2
CHUNKS = 4
MESH = pl.DeviceIdType.MESH


def kernel(
    S, T, order, acts_hbm, fresh_hbm, gain, bias, wq_hbm, wo_hbm, out, held,
    acts, wq, wo, xa, norm, qkv, attn, part, from_left, from_right, res, hop,
    acts_sem, wq_sem, wo_sem, ag_recv, ag_right, ag_left,
    rl_recv, rr_recv, rs_right, rs_left, hop_recv, hop_send,
):
    C = CHUNKS
    rows, D = xa.shape[3], xa.shape[4]
    group = T * rows
    local_heads = qkv.shape[1] // (3 * HD)
    p = lax.axis_index("tensor")
    s = lax.axis_index("section")
    last = T - 1

    barrier = pltpu.get_barrier_semaphore()
    links = ((p > 0, {"tensor": p - 1}), (p < last, {"tensor": p + 1}),
             (s > 0, {"section": s - 1}), (s < S - 1, {"section": s + 1}))
    for there, device in links:
        @pl.when(there)
        def _():
            pl.semaphore_signal(barrier, inc=1, device_id=device, device_id_type=MESH)

    acts_in = pltpu.make_async_copy(acts_hbm, acts, acts_sem)
    acts_in.start()
    wq_in = pltpu.make_async_copy(wq_hbm, wq, wq_sem)
    wq_in.start()
    wo_in = pltpu.make_async_copy(wo_hbm, wo, wo_sem)
    wo_in.start()

    @pl.when(s == 0)
    def _():
        for t in range(TICKS):
            for c in range(C):
                pltpu.make_async_copy(fresh_hbm.at[t, c], hop.at[t, c], hop_recv.at[t, c]).start()

    @pl.when(p == 0)
    def _():
        for t in range(TICKS):
            for c in range(C):
                from_left[t, c, 0] = jnp.zeros((rows, D), jnp.bfloat16)

    @pl.when(p == last)
    def _():
        for t in range(TICKS):
            for c in range(C):
                from_right[t, c, last] = jnp.zeros((rows, D), jnp.bfloat16)

    first, second = order[0], order[1]

    def gather_copy(t, c, b, right):
        sem = ag_right if right else ag_left
        return pltpu.make_async_remote_copy(
            src_ref=xa.at[t, c, b], dst_ref=xa.at[t, c, b],
            send_sem=sem.at[t, c, b], recv_sem=ag_recv.at[t, c, b],
            device_id={"tensor": p + 1 if right else p - 1}, device_id_type=MESH)

    def sum_copy(t, c, d, right):
        return pltpu.make_async_remote_copy(
            src_ref=part.at[t, c, d], dst_ref=(from_left if right else from_right).at[t, c, d],
            send_sem=(rs_right if right else rs_left).at[t, c, d],
            recv_sem=(rl_recv if right else rr_recv).at[t, c, d],
            device_id={"tensor": p + 1 if right else p - 1}, device_id_type=MESH)

    def hop_copy(t, c):
        return pltpu.make_async_remote_copy(
            src_ref=res.at[t, c], dst_ref=hop.at[t, c],
            send_sem=hop_send.at[t, c], recv_sem=hop_recv.at[t, c],
            device_id={"section": s + 1}, device_id_type=MESH)

    def gather_own(t, c):
        @pl.when(p < last)
        def _():
            gather_copy(t, c, p, True).start()

        @pl.when(p > 0)
        def _():
            gather_copy(t, c, p, False).start()

    def gather_step(t, c, j):
        b_left, b_right = p - 1 - j, p + 1 + j

        @pl.when(b_left >= 0)
        def _():
            copy = gather_copy(t, c, b_left, True)
            copy.wait_recv()

            @pl.when(p < last)
            def _():
                copy.start()

        @pl.when(b_right <= last)
        def _():
            copy = gather_copy(t, c, b_right, False)
            copy.wait_recv()

            @pl.when(p > 0)
            def _():
                copy.start()

    def project(t, c):
        for b in range(T):
            values = xa[t, c, b].astype(jnp.float32)
            centred = values - jnp.mean(values, axis=-1, keepdims=True)
            spread = jnp.mean(centred * centred, axis=-1, keepdims=True)
            norm[pl.ds(b * rows, rows), :] = (
                centred * lax.rsqrt(spread + 1e-06) * gain[...] + bias[...]
            ).astype(jnp.bfloat16)
        width = math.gcd(256, qkv.shape[1])
        r0 = pl.multiple_of(c * group, group)

        @pl.loop(0, qkv.shape[1] // width)
        def _(n):
            cols = pl.ds(pl.multiple_of(n * width, width), width)
            qkv[pl.ds(r0, group), cols] = jnp.dot(
                norm[...], wq[:, cols], preferred_element_type=jnp.float32
            ).astype(jnp.bfloat16)

    def attend(t, c):
        r0 = pl.multiple_of(c * group, group)
        for h in range(local_heads):
            at = h * 3 * HD
            q = qkv[pl.ds(r0, group), at:at + HD]
            k = qkv[:, at + HD:at + 2 * HD]
            v = qkv[:, at + 2 * HD:at + 3 * HD]
            scores = lax.dot_general(
                q, k, (((1,), (1,)), ((), ())), preferred_element_type=jnp.float32
            ) * (1.0 / math.sqrt(HD))
            top = jnp.max(scores, axis=-1, keepdims=True)
            e = jnp.exp(scores - top)
            probs = (e * (1.0 / jnp.sum(e, axis=-1, keepdims=True))).astype(jnp.bfloat16)
            attn[:, h * HD:(h + 1) * HD] = jnp.dot(
                probs, v, preferred_element_type=jnp.float32
            ).astype(jnp.bfloat16)
        width = min(512, D)
        for n in range(D // width):
            cols = slice(n * width, (n + 1) * width)
            block = jnp.dot(attn[...], wo[:, cols], preferred_element_type=jnp.float32)
            part[t, c, :, :, cols] = block.astype(jnp.bfloat16).reshape(T, rows, width)

        @pl.when(p == 0)
        def _():
            for d in range(last, 0, -1):
                sum_copy(t, c, d, True).start()

        @pl.when(p == last)
        def _():
            for d in range(last):
                sum_copy(t, c, d, False).start()

    def pass_sum(t, c, d, right):
        copy = sum_copy(t, c, d, right)
        copy.wait_recv()
        came = from_left if right else from_right
        part[t, c, d] = (
            part[t, c, d].astype(jnp.float32) + came[t, c, d].astype(jnp.float32)
        ).astype(jnp.bfloat16)
        copy.start()

    def reduce_step(t, c):
        half = T // 2
        for i in range(last):
            up, down = last - i, i

            @pl.when((p > 0) & (p < up) & (p < half))
            def _():
                pass_sum(t, c, up, True)

            @pl.when((p < last) & (p > down))
            def _():
                pass_sum(t, c, down, False)

            @pl.when((p < up) & (p >= half))
            def _():
                pass_sum(t, c, up, True)

        @pl.when(p > 0)
        def _():
            sum_copy(t, c, p, True).wait_recv()

        @pl.when(p < last)
        def _():
            sum_copy(t, c, p, False).wait_recv()
        total = (part[t, c, p].astype(jnp.float32) + from_left[t, c, p].astype(jnp.float32)
                 + from_right[t, c, p].astype(jnp.float32))
        result = (xa[t, c, p].astype(jnp.float32) + total).astype(jnp.bfloat16)
        res[t, c] = result
        out[t, c] = result

        @pl.when(s < S - 1)
        def _():
            hop_copy(t, c).start()

    def arrived(t, c):
        pltpu.make_async_copy(fresh_hbm.at[t, c], hop.at[t, c], hop_recv.at[t, c]).wait()

    acts_in.wait()
    for c in range(C):
        xa[0, c, p] = acts[first, c]
    pl.semaphore_wait(barrier, sum(there.astype(jnp.int32) for there, _ in links))
    for c in range(C):
        gather_own(0, c)
    for j in range(last - 1):
        for c in range(C):
            gather_step(0, c, j)
    wq_in.wait()
    for c in range(C):
        gather_step(0, c, last - 1)
        project(0, c)
    wo_in.wait()

    @pl.loop(0, C)
    def _(c):
        attend(0, c)

    for slot in range(C + last + 1):
        if slot < C:
            reduce_step(0, slot)
        c = slot - 1
        if 0 <= c < C:
            arrived(0, c)
            xa[1, c, p] = jnp.where(first == second, hop[0, c], acts[second, c])
            gather_own(1, c)
        for j in range(last):
            c = slot - 2 - j
            if 0 <= c < C:
                gather_step(1, c, j)
        c = slot - 1 - last
        if 0 <= c < C:
            project(1, c)

    @pl.loop(0, C)
    def _(c):
        attend(1, c)

    for c in range(C):
        reduce_step(1, c)
    for c in range(C):
        arrived(1, c)
        for j in range(2):
            held[j, c] = jnp.where(
                second == j, hop[1, c], jnp.where(first == j, hop[0, c], acts[j, c]))

    for t in range(TICKS):
        @pl.loop(0, C)
        def _(c):
            for b in range(T):
                @pl.when((p < last) & (p >= b))
                def _():
                    gather_copy(t, c, b, True).wait_send()

                @pl.when((p > 0) & (p <= b))
                def _():
                    gather_copy(t, c, b, False).wait_send()

                @pl.when(p < b)
                def _():
                    sum_copy(t, c, b, True).wait_send()

                @pl.when(p > b)
                def _():
                    sum_copy(t, c, b, False).wait_send()

            @pl.when(s < S - 1)
            def _():
                hop_copy(t, c).wait_send()


def body(acts, fresh, order, ln_gain, ln_bias, wqkv, wo):
    S, T = lax.axis_size("section"), lax.axis_size("tensor")
    slots, tokens, D = acts.shape[1:]
    rows = tokens // CHUNKS
    cols = wqkv.shape[2]
    vmem = pl.BlockSpec(memory_space=pltpu.VMEM)
    hbm = pl.BlockSpec(memory_space=pl.ANY)
    block = (TICKS, CHUNKS, rows, D)
    wide = (TICKS, CHUNKS, T, rows, D)
    sem = lambda *shape: pltpu.SemaphoreType.DMA(shape)
    out, held = pl.pallas_call(
        functools.partial(kernel, S, T),
        name="relay",
        out_shape=(jax.ShapeDtypeStruct(block, jnp.bfloat16),) * 2,
        in_specs=[pl.BlockSpec(memory_space=pltpu.SMEM), hbm, hbm, vmem, vmem, hbm, hbm],
        out_specs=(vmem, vmem),
        scratch_shapes=[
            pltpu.VMEM(block, jnp.bfloat16),
            pltpu.VMEM((D, cols), jnp.bfloat16),
            pltpu.VMEM(wo.shape[1:], jnp.bfloat16),
            pltpu.VMEM(wide, jnp.bfloat16),
            pltpu.VMEM((T * rows, D), jnp.bfloat16),
            pltpu.VMEM((T * tokens, cols), jnp.bfloat16),
            pltpu.VMEM((T * rows, cols // 3), jnp.bfloat16),
            pltpu.VMEM(wide, jnp.bfloat16),
            pltpu.VMEM(wide, jnp.bfloat16),
            pltpu.VMEM(wide, jnp.bfloat16),
            pltpu.VMEM(block, jnp.bfloat16),
            pltpu.VMEM(block, jnp.bfloat16),
            pltpu.SemaphoreType.DMA, pltpu.SemaphoreType.DMA, pltpu.SemaphoreType.DMA,
            sem(TICKS, CHUNKS, T), sem(TICKS, CHUNKS, T), sem(TICKS, CHUNKS, T),
            sem(TICKS, CHUNKS, T), sem(TICKS, CHUNKS, T),
            sem(TICKS, CHUNKS, T), sem(TICKS, CHUNKS, T),
            sem(TICKS, CHUNKS), sem(TICKS, CHUNKS),
        ],
        compiler_params=pltpu.CompilerParams(collective_id=0, has_side_effects=True),
    )(
        order[0], acts.reshape(slots, CHUNKS, rows, D), fresh.reshape(TICKS, CHUNKS, rows, D),
        ln_gain, ln_bias, wqkv[0], wo[0],
    )
    return out.reshape(TICKS, 1, tokens, D), held.reshape(1, slots, tokens, D)


def solution(mesh):
    return jax.shard_map(
        body,
        mesh=mesh,
        in_specs=(
            P("section", "dp", "tensor", None),
            P("dp", "tensor", None),
            P("section", None),
            P("section", None),
            P("section", None),
            P("section", None, "tensor"),
            P("section", "tensor", None),
        ),
        out_specs=(P("dp", "section", "tensor", None), P("section", "dp", "tensor", None)),
        check_vma=False,
    )
```

```python
import functools
import math

import jax
import jax.numpy as jnp
from jax import lax
from jax.experimental import pallas as pl
from jax.experimental.pallas import tpu as pltpu
from jax.sharding import PartitionSpec as P

HD = 128
TICKS = 2
CHUNKS = 8
ATTEND = 2
PROJECT = 4
MESH = pl.DeviceIdType.MESH


def plan(T, C, steps, queue):
    last, per = T - 1, C // steps
    wire, reach, hop_wire, hop_reach = 5.64 / C, 2.2, 2.82 / C, 2.6
    add, norm, attend, project = 0.5 / C, 0.8 / C, 1.0, 2.0
    clock, free, arrivals = [0.0] * T, {}, {}

    def send(link, key, at, wire=wire, reach=reach):
        free[link] = max(at, free.get(link, 0.0)) + wire
        arrivals[key] = free[link] + reach

    orders = []
    for t in range(TICKS):
        for p in range(T):
            for k in range(steps):
                clock[p] += attend
                for q, (c, d) in queue(t, k):
                    if p == q:
                        send((p, d > p), ("sum", t, p + 1 if d > p else p - 1, c, d, d > p), clock[p])
        todo, order = [], [[] for _ in range(T)]
        for p in range(T):
            todo.append([("up", c, d) for c in range(C) for d in range(p + 1, T) if p > 0]
                        + [("down", c, d) for c in range(C) for d in range(p) if p < last]
                        + [("own", c, p) for c in range(C)] + [("next", c, p) for c in range(C)])
            if t == 0:
                todo[p] += [("left", c, b) for c in range(C) for b in range(p)]
                todo[p] += [("right", c, b) for c in range(C) for b in range(p + 1, T)]
                todo[p] += [("project", k, p) for k in range(C // PROJECT)]
        sums = ("up", "down", "own")
        rank = {"up": 0, "down": 0, "own": 1, "next": 2, "left": 3, "right": 3, "project": 4}

        def ready(p, kind, c, d):
            need = []
            if kind == "up" or (kind == "own" and p > 0):
                need.append(("sum", t, p, c, d, True))
            if kind == "down" or (kind == "own" and p < last):
                need.append(("sum", t, p, c, d, False))
            if kind == "next":
                need.append(("hop", t, p, c))
                if c == C - 1 and any(e[0] in sums for e in todo[p]):
                    return None
            if kind in ("left", "right"):
                need.append(("gather", p, c, d))
            if kind == "project" and any(
                    e[0] in ("next", "left", "right") and e[1] // PROJECT == c for e in todo[p]):
                return None
            times = [arrivals.get(key) for key in need]
            return None if None in times else max([clock[p]] + times)

        while any(todo):
            at, _, c, p, (kind, c, d) = min(
                (ready(p, *e), rank[e[0]], e[1], p, e)
                for p in range(T) for e in todo[p] if ready(p, *e) is not None)
            todo[p].remove((kind, c, d))
            order[p].append((kind, c, d))
            if kind in ("up", "down"):
                up = kind == "up"
                at += add
                send((p, up), ("sum", t, p + 1 if up else p - 1, c, d, up), at)
            elif kind == "own":
                at += add
                send((p, "hop"), ("hop", t, p, c), at, hop_wire, hop_reach)
            elif kind == "project":
                at += project
            elif t == 0:
                if kind in ("next", "left") and p < last:
                    send((p, True), ("gather", p + 1, c, d), at)
                if kind in ("next", "right") and p > 0:
                    send((p, False), ("gather", p - 1, c, d), at)
                at += norm
            clock[p] = at
        orders.append(order)
    return orders


def edge_queue(T, C, steps):
    last, per = T - 1, C // steps

    def queue(t, k):
        ends = [(0, list(range(last, 0, -1))), (last, list(range(last)))]
        sends = [(p, (c, far[0])) for p, far in ends for c in range(k * per, (k + 1) * per)]
        if k == steps - 1:
            for p, far in ends:
                rest = [(c, d) for c in range(C) for d in far[1:]]
                if t == TICKS - 1:
                    rest = [(c, d) for d in far[1:] for c in range(C)]
                sends += [(p, e) for e in rest]
        return sends

    return queue


def kernel(
    S, T, order_hbm, acts_hbm, fresh_hbm, gain_hbm, bias_hbm, wq_hbm, wo_hbm, out, held,
    order, acts, gain, bias, wq, wo, xa, norm, qkv, attn, part, from_left, from_right, res, hop,
    order_sem, acts_sem, gain_sem, bias_sem, wq_sem, wo_sem, ag_recv, rl_recv, rr_recv,
    sent_right, sent_left, hop_recv, hop_sent,
):
    C = CHUNKS
    rows, D = xa.shape[3], xa.shape[4]
    group = T * rows
    local_heads = qkv.shape[1] // (3 * HD)
    p = lax.axis_index("tensor")
    s = lax.axis_index("section")
    last = T - 1
    steps = C // ATTEND
    per = ATTEND
    queue = edge_queue(T, C, steps)
    orders = plan(T, C, steps, queue)

    barrier = pltpu.get_barrier_semaphore()
    links = ((p > 0, {"tensor": p - 1}), (p < last, {"tensor": p + 1}),
             (s > 0, {"section": s - 1}), (s < S - 1, {"section": s + 1}))
    for there, device in links:
        @pl.when(there)
        def _():
            pl.semaphore_signal(barrier, inc=1, device_id=device, device_id_type=MESH)

    order_in = pltpu.make_async_copy(order_hbm, order, order_sem)
    acts_in = pltpu.make_async_copy(acts_hbm, acts, acts_sem)
    gain_in = pltpu.make_async_copy(gain_hbm, gain, gain_sem)
    bias_in = pltpu.make_async_copy(bias_hbm, bias, bias_sem)
    wq_in = pltpu.make_async_copy(wq_hbm, wq, wq_sem)
    wo_in = pltpu.make_async_copy(wo_hbm, wo, wo_sem)
    for copy in (order_in, acts_in, gain_in, bias_in, wq_in, wo_in):
        copy.start()

    @pl.when(s == 0)
    def _():
        for t in range(TICKS):
            for c in range(C):
                pltpu.make_async_copy(fresh_hbm.at[t, c], hop.at[t, c], hop_recv.at[t, c]).start()

    def scoped(name):
        return lambda f: jax.named_scope(name)(f)

    def gather_copy(t, c, b, right):
        return pltpu.make_async_remote_copy(
            src_ref=xa.at[t, c, b], dst_ref=xa.at[t, c, b],
            send_sem=(sent_right if right else sent_left).at[t], recv_sem=ag_recv.at[t, c, b],
            device_id={"tensor": p + 1 if right else p - 1}, device_id_type=MESH)

    def sum_copy(t, c, d, right):
        return pltpu.make_async_remote_copy(
            src_ref=part.at[t, c, d], dst_ref=(from_left if right else from_right).at[t, c, d],
            send_sem=(sent_right if right else sent_left).at[t],
            recv_sem=(rl_recv if right else rr_recv).at[c, d],
            device_id={"tensor": p + 1 if right else p - 1}, device_id_type=MESH)

    def hop_copy(t, c):
        return pltpu.make_async_remote_copy(
            src_ref=res.at[t, c], dst_ref=hop.at[t, c],
            send_sem=hop_sent.at[t], recv_sem=hop_recv.at[t, c],
            device_id={"section": s + 1}, device_id_type=MESH)

    @scoped("gather_own")
    def gather_own(t, c):
        @pl.when(p < last)
        def _():
            gather_copy(t, c, p, True).start()

        @pl.when(p > 0)
        def _():
            gather_copy(t, c, p, False).start()

    @scoped("normed")
    def normed(t, c, b):
        values = xa[t, c, b].astype(jnp.float32)
        centred = values - jnp.mean(values, axis=-1, keepdims=True)
        spread = jnp.mean(centred * centred, axis=-1, keepdims=True)
        norm[c, b] = (
            centred * lax.rsqrt(spread + 1e-06) * gain[...] + bias[...]
        ).astype(jnp.bfloat16)

    @scoped("gather_step")
    def gather_step(t, c, j):
        b_left, b_right = p - 1 - j, p + 1 + j

        @pl.when(b_left >= 0)
        def _():
            copy = gather_copy(t, c, b_left, True)
            copy.wait_recv()

            @pl.when(p < last)
            def _():
                copy.start()

        @pl.when(b_right <= last)
        def _():
            copy = gather_copy(t, c, b_right, False)
            copy.wait_recv()

            @pl.when(p > 0)
            def _():
                copy.start()

        @pl.when(b_left >= 0)
        def _():
            normed(t, c, b_left)

        @pl.when(b_right <= last)
        def _():
            normed(t, c, b_right)

    @scoped("project")
    def project(part_of):
        width = math.gcd(256, qkv.shape[1])
        span = PROJECT * group

        @pl.loop(0, qkv.shape[1] // width)
        def _(n):
            cols = pl.ds(pl.multiple_of(n * width, width), width)
            qkv[part_of * span:(part_of + 1) * span, cols] = jnp.dot(
                norm[PROJECT * part_of:PROJECT * (part_of + 1)].reshape(span, D), wq[:, cols],
                preferred_element_type=jnp.float32,
            ).astype(jnp.bfloat16)

    @scoped("attend")
    def attend(t, part_of):
        span = ATTEND * group
        r0 = pl.multiple_of(part_of * span, span)
        heads = range(local_heads)

        def columns(h, j):
            return slice((h * 3 + j) * HD, (h * 3 + j + 1) * HD)

        scores = [lax.dot_general(
            qkv[pl.ds(r0, span), columns(h, 0)], qkv[:, columns(h, 1)],
            (((1,), (1,)), ((), ())), preferred_element_type=jnp.float32) for h in heads]
        scores = [x * (1.0 / math.sqrt(HD)) for x in scores]
        tops = [jnp.max(x, axis=-1, keepdims=True) for x in scores]
        powers = [jnp.exp(x - top) for x, top in zip(scores, tops)]
        sums = [jnp.sum(x, axis=-1, keepdims=True) for x in powers]
        probs = [(x * (1.0 / total)).astype(jnp.bfloat16) for x, total in zip(powers, sums)]
        mixed = [jnp.dot(probs[h], qkv[:, columns(h, 2)], preferred_element_type=jnp.float32)
                 for h in heads]
        for h in heads:
            attn[:, h * HD:(h + 1) * HD] = mixed[h].astype(jnp.bfloat16)
        width = min(512, D)
        for n in range(D // width):
            cols = slice(n * width, (n + 1) * width)
            block = jnp.dot(attn[...], wo[:, cols], preferred_element_type=jnp.float32)
            block = block.reshape(ATTEND, T, rows, width).astype(jnp.bfloat16)
            part[t, pl.ds(part_of * ATTEND, ATTEND), :, :, cols] = block
        for c in range(ATTEND):
            c += part_of * ATTEND

            @pl.when(p == 0)
            def _():
                sum_copy(t, c, last, True).start()

            @pl.when(p == last)
            def _():
                sum_copy(t, c, 0, False).start()

    def send_rest(t):
        for q in (0, last):
            @pl.when(p == q)
            def _():
                for end, (c, d) in queue(t, steps - 1)[2 * per:]:
                    if end == q:
                        sum_copy(t, c, d, q == 0).start()

    def pass_sum(t, c, d, right):
        copy = sum_copy(t, c, d, right)
        copy.wait_recv()
        came = from_left if right else from_right
        part[t, c, d] = (
            part[t, c, d].astype(jnp.float32) + came[t, c, d].astype(jnp.float32)
        ).astype(jnp.bfloat16)
        copy.start()

    @scoped("sum_own")
    def sum_own(t, c, q):
        total = part[t, c, q].astype(jnp.float32)
        if q > 0:
            sum_copy(t, c, q, True).wait_recv()
            total += from_left[t, c, q].astype(jnp.float32)
        if q < last:
            sum_copy(t, c, q, False).wait_recv()
            total += from_right[t, c, q].astype(jnp.float32)
        result = (xa[t, c, q].astype(jnp.float32) + total).astype(jnp.bfloat16)
        res[t, c] = result

        @pl.when(s < S - 1)
        def _():
            hop_copy(t, c).start()
        out[t, c] = result

    @scoped("arrived")
    def arrived(t, c):
        pltpu.make_async_copy(fresh_hbm.at[t, c], hop.at[t, c], hop_recv.at[t, c]).wait()

    def drain(t):
        for right, there in ((True, p < last), (False, p > 0)):
            @pl.when(there)
            def _():
                pltpu.make_async_remote_copy(
                    src_ref=xa.at[t], dst_ref=xa.at[t],
                    send_sem=(sent_right if right else sent_left).at[t], recv_sem=ag_recv.at[t, 0, 0],
                    device_id={"tensor": p + 1 if right else p - 1}, device_id_type=MESH,
                ).wait_send()

        @pl.when(s < S - 1)
        def _():
            pltpu.make_async_remote_copy(
                src_ref=res.at[t], dst_ref=hop.at[t],
                send_sem=hop_sent.at[t], recv_sem=hop_recv.at[t, 0],
                device_id={"section": s + 1}, device_id_type=MESH).wait_send()

    def step(t, q, kind, c, d):
        if kind in ("up", "down"):
            with jax.named_scope("pass_sum"):
                pass_sum(t, c, d, kind == "up")
        elif kind == "own":
            sum_own(t, c, q)
        elif kind == "project":
            project(c)
        elif kind == "next" and t == 0:
            arrived(0, c)
            xa[1, c, q] = jnp.where(first == second, hop[0, c], acts[second, c])
            if q < last:
                gather_copy(1, c, q, True).start()
            if q > 0:
                gather_copy(1, c, q, False).start()
            normed(1, c, q)
        elif kind == "next":
            arrived(1, c)
            for j in range(2):
                held[j, c] = jnp.where(
                    second == j, hop[1, c], jnp.where(first == j, hop[0, c], acts[j, c]))
        else:
            with jax.named_scope("gather_step"):
                copy = gather_copy(1, c, d, kind == "left")
                copy.wait_recv()
                if (q < last) if kind == "left" else (q > 0):
                    copy.start()
            normed(1, c, d)

    with jax.named_scope("acts_wait"):
        order_in.wait()
        acts_in.wait()
    first, second = order[0, 0], order[0, 1]
    for c in range(C):
        xa[0, c, p] = acts[first, c]
    with jax.named_scope("entry"):
        pl.semaphore_wait(barrier, sum(there.astype(jnp.int32) for there, _ in links))
    for c in range(C):
        gather_own(0, c)

    gain_in.wait()
    bias_in.wait()
    for c in range(C):
        normed(0, c, p)
    for j in range(last - 1):
        for c in range(C):
            gather_step(0, c, j)
    wq_in.wait()
    for c in range(C):
        gather_step(0, c, last - 1)
        if c % PROJECT == PROJECT - 1:
            project(c // PROJECT)
    wo_in.wait()

    for t in range(TICKS):
        @pl.loop(0, steps)
        def _(part_of):
            attend(t, part_of)

        send_rest(t)
        for q in range(T):
            @pl.when(p == q)
            def _():
                for event in orders[t][q]:
                    step(t, q, *event)
        with jax.named_scope("drain"):
            drain(t)


def store(out, held, out_hbm, held_hbm, out_sem, held_sem):
    copies = (pltpu.make_async_copy(out, out_hbm, out_sem),
              pltpu.make_async_copy(held, held_hbm, held_sem))
    for copy in copies:
        copy.start()
    for copy in copies:
        copy.wait()


def body(acts, fresh, order, ln_gain, ln_bias, wqkv, wo):
    S, T = lax.axis_size("section"), lax.axis_size("tensor")
    slots, tokens, D = acts.shape[1:]
    rows = tokens // CHUNKS
    cols = wqkv.shape[2]
    vmem = pl.BlockSpec(memory_space=pltpu.VMEM)
    hbm = pl.BlockSpec(memory_space=pltpu.HBM)
    block = (TICKS, CHUNKS, rows, D)
    wide = (TICKS, CHUNKS, T, rows, D)
    sem = lambda *shape: pltpu.SemaphoreType.DMA(shape)
    out, held = pl.pallas_call(
        functools.partial(kernel, S, T),
        name="relay",
        out_shape=(jax.ShapeDtypeStruct(block, jnp.bfloat16),) * 2,
        in_specs=[hbm, hbm, hbm, hbm, hbm, hbm, hbm],
        out_specs=(vmem, vmem),
        scratch_shapes=[
            pltpu.SMEM(order.shape, jnp.int32),
            pltpu.VMEM(block, jnp.bfloat16),
            pltpu.VMEM((1, D), jnp.float32),
            pltpu.VMEM((1, D), jnp.float32),
            pltpu.VMEM((D, cols), jnp.bfloat16),
            pltpu.VMEM(wo.shape[1:], jnp.bfloat16),
            pltpu.VMEM(wide, jnp.bfloat16),
            pltpu.VMEM((CHUNKS, T, rows, D), jnp.bfloat16),
            pltpu.VMEM((T * tokens, cols), jnp.bfloat16),
            pltpu.VMEM((ATTEND * T * rows, cols // 3), jnp.bfloat16),
            pltpu.VMEM(wide, jnp.bfloat16),
            pltpu.VMEM(wide, jnp.bfloat16),
            pltpu.VMEM(wide, jnp.bfloat16),
            pltpu.VMEM(block, jnp.bfloat16),
            pltpu.VMEM(block, jnp.bfloat16),
            *[pltpu.SemaphoreType.DMA] * 6,
            sem(TICKS, CHUNKS, T), sem(CHUNKS, T), sem(CHUNKS, T),
            sem(TICKS), sem(TICKS), sem(TICKS, CHUNKS), sem(TICKS),
        ],
        compiler_params=pltpu.CompilerParams(
            collective_id=0, has_side_effects=True, vmem_limit_bytes=32 << 20),
    )(*(pltpu.with_memory_space_constraint(x, pltpu.HBM) for x in (
        order, acts.reshape(slots, CHUNKS, rows, D), fresh.reshape(TICKS, CHUNKS, rows, D),
        ln_gain, ln_bias, wqkv[0], wo[0],
    )))
    out, held = pl.pallas_call(
        store, name="store",
        out_shape=(jax.ShapeDtypeStruct(block, jnp.bfloat16),) * 2,
        in_specs=[vmem, vmem], out_specs=(hbm, hbm),
        scratch_shapes=[pltpu.SemaphoreType.DMA, pltpu.SemaphoreType.DMA],
        compiler_params=pltpu.CompilerParams(vmem_limit_bytes=4 << 20),
    )(out, held)
    return out.reshape(TICKS, 1, tokens, D), held.reshape(1, slots, tokens, D)


def solution(mesh):
    return jax.shard_map(
        body,
        mesh=mesh,
        in_specs=(
            P("section", "dp", "tensor", None),
            P("dp", "tensor", None),
            P("section", None),
            P("section", None),
            P("section", None),
            P("section", None, "tensor"),
            P("section", "tensor", None),
        ),
        out_specs=(P("dp", "section", "tensor", None), P("section", "dp", "tensor", None)),
        check_vma=False,
    )
```

```python
import functools
import math

import jax
import jax.numpy as jnp
from jax import lax
from jax.experimental import pallas as pl
from jax.experimental.pallas import tpu as pltpu
from jax.sharding import PartitionSpec as P

HD = 128
TICKS = 2
CHUNKS = 8
ATTEND = 2
PROJECT = 4
MESH = pl.DeviceIdType.MESH


def plan(T, C, steps, queue):
    last, per = T - 1, C // steps
    wire, reach, hop_wire, hop_reach = 5.64 / C, 2.2, 2.82 / C, 2.6
    add, norm, attend, project = 0.5 / C, 0.8 / C, 1.0, 1.7
    clock, free, arrivals = [0.0] * T, {}, {}

    def send(link, key, at, wire=wire, reach=reach):
        free[link] = max(at, free.get(link, 0.0)) + wire
        arrivals[key] = free[link] + reach

    orders = []
    for t in range(TICKS):
        for p in range(T):
            for k in range(steps):
                clock[p] += attend
                for q, (c, d) in queue(t, k):
                    if p == q:
                        send((p, d > p), ("sum", t, p + 1 if d > p else p - 1, c, d, d > p), clock[p])
        todo, order = [], [[] for _ in range(T)]
        for p in range(T):
            todo.append([("up", c, d) for c in range(C) for d in range(p + 1, T) if p > 0]
                        + [("down", c, d) for c in range(C) for d in range(p) if p < last]
                        + [("own", c, p) for c in range(C)] + [("next", c, p) for c in range(C)])
            if t == 0:
                todo[p] += [("left", c, b) for c in range(C) for b in range(p)]
                todo[p] += [("right", c, b) for c in range(C) for b in range(p + 1, T)]
                todo[p] += [("project", k, p) for k in range(C // PROJECT)]
        sums = ("up", "down", "own")
        rank = {"up": 0, "down": 0, "own": 1, "next": 2, "left": 3, "right": 3, "project": 4}

        def ready(p, kind, c, d):
            need = []
            if kind == "up" or (kind == "own" and p > 0):
                need.append(("sum", t, p, c, d, True))
            if kind == "down" or (kind == "own" and p < last):
                need.append(("sum", t, p, c, d, False))
            if kind == "next":
                need.append(("hop", t, p, c))
                if c == C - 1 and any(e[0] in sums for e in todo[p]):
                    return None
            if kind in ("left", "right"):
                need.append(("gather", p, c, d))
            if kind == "project" and any(
                    e[0] in ("next", "left", "right") and e[1] // PROJECT == c for e in todo[p]):
                return None
            times = [arrivals.get(key) for key in need]
            return None if None in times else max([clock[p]] + times)

        while any(todo):
            at, _, c, p, (kind, c, d) = min(
                (ready(p, *e), rank[e[0]], e[1], p, e)
                for p in range(T) for e in todo[p] if ready(p, *e) is not None)
            todo[p].remove((kind, c, d))
            order[p].append((kind, c, d))
            if kind in ("up", "down"):
                up = kind == "up"
                at += add
                send((p, up), ("sum", t, p + 1 if up else p - 1, c, d, up), at)
            elif kind == "own":
                at += add
                send((p, "hop"), ("hop", t, p, c), at, hop_wire, hop_reach)
            elif kind == "project":
                at += project
            elif t == 0:
                if kind in ("next", "left") and p < last:
                    send((p, True), ("gather", p + 1, c, d), at)
                if kind in ("next", "right") and p > 0:
                    send((p, False), ("gather", p - 1, c, d), at)
                at += norm
            clock[p] = at
        orders.append(order)
    return orders


def edge_queue(T, C, steps):
    last, per = T - 1, C // steps
    lead = (0, 5, 7)

    def queue(t, k):
        turns = [(i, c) if t == TICKS - 1 else (c + lead[i], -i, c) for c in range(C) for i in range(last)]
        turns = sorted(zip(turns, [(c, i) for c in range(C) for i in range(last)]))
        at, sends = 0, []
        for _, (c, i) in turns:
            at = max(at, c // per)
            if at == k:
                sends += [(0, (c, last - i)), (last, (c, i))]
        return sends

    return queue


def kernel(
    S, T, order_hbm, acts_hbm, fresh_hbm, gain_hbm, bias_hbm, wq_hbm, wo_hbm, out, held,
    order, acts, gain, bias, wq, wo, xa, norm, qkv, attn, part, from_left, from_right, res, hop,
    order_sem, acts_sem, gain_sem, bias_sem, wq_sem, wo_sem, ag_recv, rl_recv, rr_recv,
    sent_right, sent_left, hop_recv, hop_sent,
):
    C = CHUNKS
    rows, D = xa.shape[3], xa.shape[4]
    group = T * rows
    local_heads = qkv.shape[1] // (3 * HD)
    p = lax.axis_index("tensor")
    s = lax.axis_index("section")
    last = T - 1
    steps = C // ATTEND
    queue = edge_queue(T, C, steps)
    orders = plan(T, C, steps, queue)

    barrier = pltpu.get_barrier_semaphore()
    links = ((p > 0, {"tensor": p - 1}), (p < last, {"tensor": p + 1}),
             (s > 0, {"section": s - 1}), (s < S - 1, {"section": s + 1}))
    for there, device in links:
        @pl.when(there)
        def _():
            pl.semaphore_signal(barrier, inc=1, device_id=device, device_id_type=MESH)

    order_in = pltpu.make_async_copy(order_hbm, order, order_sem)
    acts_in = pltpu.make_async_copy(acts_hbm, acts, acts_sem)
    gain_in = pltpu.make_async_copy(gain_hbm, gain, gain_sem)
    bias_in = pltpu.make_async_copy(bias_hbm, bias, bias_sem)
    wq_in = pltpu.make_async_copy(wq_hbm, wq, wq_sem)
    wo_in = pltpu.make_async_copy(wo_hbm, wo, wo_sem)
    for copy in (order_in, acts_in, gain_in, bias_in, wq_in, wo_in):
        copy.start()

    @pl.when(s == 0)
    def _():
        for t in range(TICKS):
            for c in range(C):
                pltpu.make_async_copy(fresh_hbm.at[t, c], hop.at[t, c], hop_recv.at[t, c]).start()

    def scoped(name):
        return lambda f: jax.named_scope(name)(f)

    def gather_copy(t, c, b, right):
        return pltpu.make_async_remote_copy(
            src_ref=xa.at[t, c, b], dst_ref=xa.at[t, c, b],
            send_sem=(sent_right if right else sent_left).at[t], recv_sem=ag_recv.at[t, c, b],
            device_id={"tensor": p + 1 if right else p - 1}, device_id_type=MESH)

    def sum_copy(t, c, d, right):
        return pltpu.make_async_remote_copy(
            src_ref=part.at[t, c, d], dst_ref=(from_left if right else from_right).at[t, c, d],
            send_sem=(sent_right if right else sent_left).at[t],
            recv_sem=rl_recv.at[c, d - 1] if right else rr_recv.at[c, d],
            device_id={"tensor": p + 1 if right else p - 1}, device_id_type=MESH)

    def hop_copy(t, c):
        return pltpu.make_async_remote_copy(
            src_ref=res.at[t, c], dst_ref=hop.at[t, c],
            send_sem=hop_sent.at[t], recv_sem=hop_recv.at[t, c],
            device_id={"section": s + 1}, device_id_type=MESH)

    @scoped("gather_own")
    def gather_own(t, c):
        @pl.when(p < last)
        def _():
            gather_copy(t, c, p, True).start()

        @pl.when(p > 0)
        def _():
            gather_copy(t, c, p, False).start()

    @scoped("normed")
    def normed(t, c, b):
        values = xa[t, c, b].astype(jnp.float32)
        centred = values - jnp.mean(values, axis=-1, keepdims=True)
        spread = jnp.mean(centred * centred, axis=-1, keepdims=True)
        norm[c, b] = (
            centred * lax.rsqrt(spread + 1e-06) * gain[...] + bias[...]
        ).astype(jnp.bfloat16)

    @scoped("gather_step")
    def gather_step(t, c, j):
        b_left, b_right = p - 1 - j, p + 1 + j

        @pl.when(b_left >= 0)
        def _():
            copy = gather_copy(t, c, b_left, True)
            copy.wait_recv()

            @pl.when(p < last)
            def _():
                copy.start()

        @pl.when(b_right <= last)
        def _():
            copy = gather_copy(t, c, b_right, False)
            copy.wait_recv()

            @pl.when(p > 0)
            def _():
                copy.start()

        @pl.when(b_left >= 0)
        def _():
            normed(t, c, b_left)

        @pl.when(b_right <= last)
        def _():
            normed(t, c, b_right)

    @scoped("project")
    def project(part_of, begin, width):
        span = PROJECT * group

        @pl.loop(0, local_heads)
        def _(h):
            cols = pl.ds(pl.multiple_of(h * (3 * HD), HD) + begin, width)
            qkv[part_of * span:(part_of + 1) * span, cols] = jnp.dot(
                norm[PROJECT * part_of:PROJECT * (part_of + 1)].reshape(span, D), wq[:, cols],
                preferred_element_type=jnp.float32,
            ).astype(jnp.bfloat16)

    def project_keys(part_of):
        project(part_of, HD, 2 * HD)

    def project_queries(part_of):
        project(part_of, 0, HD)

    def project_part(part_of):
        project_keys(part_of)
        if part_of < C // PROJECT - 1:
            project_queries(part_of)

    def attend_all(t):
        half = steps // (C // PROJECT)

        for part in range(C // PROJECT):
            @pl.loop(part * half, (part + 1) * half)
            def _(k):
                attend(t, k)

            if part == C // PROJECT - 2:
                project_queries(part + 1)

    @scoped("attend")
    def attend(t, part_of):
        span = ATTEND * group
        r0 = pl.multiple_of(part_of * span, span)
        heads = range(local_heads)

        def columns(h, j):
            return slice((h * 3 + j) * HD, (h * 3 + j + 1) * HD)

        scores = [lax.dot_general(
            qkv[pl.ds(r0, span), columns(h, 0)], qkv[:, columns(h, 1)],
            (((1,), (1,)), ((), ())), preferred_element_type=jnp.float32) for h in heads]
        scores = [x * (1.0 / math.sqrt(HD)) for x in scores]
        tops = [jnp.max(x, axis=-1, keepdims=True) for x in scores]
        powers = [jnp.exp(x - top) for x, top in zip(scores, tops)]
        sums = [jnp.sum(x, axis=-1, keepdims=True) for x in powers]
        probs = [(x * (1.0 / total)).astype(jnp.bfloat16) for x, total in zip(powers, sums)]
        mixed = [jnp.dot(probs[h], qkv[:, columns(h, 2)], preferred_element_type=jnp.float32)
                 for h in heads]
        for h in heads:
            attn[:, h * HD:(h + 1) * HD] = mixed[h].astype(jnp.bfloat16)
        width = min(512, D)
        for n in range(D // width):
            cols = slice(n * width, (n + 1) * width)
            block = jnp.dot(attn[...], wo[:, cols], preferred_element_type=jnp.float32)
            block = block.reshape(ATTEND, T, rows, width).astype(jnp.bfloat16)
            part[t, pl.ds(part_of * ATTEND, ATTEND), :, :, cols] = block
        for k in range(steps):
            for q in (0, last):
                @pl.when((part_of == k) & (p == q))
                def _():
                    for end, (c, d) in queue(t, k):
                        if end == q:
                            sum_copy(t, c, d, q == 0).start()

    def pass_sum(t, c, d, right):
        copy = sum_copy(t, c, d, right)
        copy.wait_recv()
        came = from_left if right else from_right
        part[t, c, d] = (
            part[t, c, d].astype(jnp.float32) + came[t, c, d].astype(jnp.float32)
        ).astype(jnp.bfloat16)
        copy.start()

    @scoped("sum_own")
    def sum_own(t, c, q):
        total = part[t, c, q].astype(jnp.float32)
        if q > 0:
            sum_copy(t, c, q, True).wait_recv()
            total += from_left[t, c, q].astype(jnp.float32)
        if q < last:
            sum_copy(t, c, q, False).wait_recv()
            total += from_right[t, c, q].astype(jnp.float32)
        result = (xa[t, c, q].astype(jnp.float32) + total).astype(jnp.bfloat16)
        res[t, c] = result

        @pl.when(s < S - 1)
        def _():
            hop_copy(t, c).start()
        out[t, c] = result

    @scoped("arrived")
    def arrived(t, c):
        pltpu.make_async_copy(fresh_hbm.at[t, c], hop.at[t, c], hop_recv.at[t, c]).wait()

    def drain(t):
        for right, there in ((True, p < last), (False, p > 0)):
            @pl.when(there)
            def _():
                pltpu.make_async_remote_copy(
                    src_ref=xa.at[t], dst_ref=xa.at[t],
                    send_sem=(sent_right if right else sent_left).at[t], recv_sem=ag_recv.at[t, 0, 0],
                    device_id={"tensor": p + 1 if right else p - 1}, device_id_type=MESH,
                ).wait_send()

        @pl.when(s < S - 1)
        def _():
            pltpu.make_async_remote_copy(
                src_ref=res.at[t], dst_ref=hop.at[t],
                send_sem=hop_sent.at[t], recv_sem=hop_recv.at[t, 0],
                device_id={"section": s + 1}, device_id_type=MESH).wait_send()

    def step(t, q, kind, c, d):
        if kind in ("up", "down"):
            with jax.named_scope("pass_sum"):
                pass_sum(t, c, d, kind == "up")
        elif kind == "own":
            sum_own(t, c, q)
        elif kind == "project":
            project_part(c)
        elif kind == "next" and t == 0:
            arrived(0, c)
            xa[1, c, q] = jnp.where(first == second, hop[0, c], acts[second, c])
            if q < last:
                gather_copy(1, c, q, True).start()
            if q > 0:
                gather_copy(1, c, q, False).start()
            normed(1, c, q)
        elif kind == "next":
            arrived(1, c)
            for j in range(2):
                held[j, c] = jnp.where(
                    second == j, hop[1, c], jnp.where(first == j, hop[0, c], acts[j, c]))
        else:
            with jax.named_scope("gather_step"):
                copy = gather_copy(1, c, d, kind == "left")
                copy.wait_recv()
                if (q < last) if kind == "left" else (q > 0):
                    copy.start()
            normed(1, c, d)

    with jax.named_scope("acts_wait"):
        order_in.wait()
        acts_in.wait()
    first, second = order[0, 0], order[0, 1]
    for c in range(C):
        xa[0, c, p] = acts[first, c]
    with jax.named_scope("entry"):
        pl.semaphore_wait(barrier, sum(there.astype(jnp.int32) for there, _ in links))
    for c in range(C):
        gather_own(0, c)

    gain_in.wait()
    bias_in.wait()
    for c in range(C):
        normed(0, c, p)
    for j in range(last - 1):
        for c in range(C):
            gather_step(0, c, j)
    wq_in.wait()
    for c in range(C):
        gather_step(0, c, last - 1)
        if c % PROJECT == PROJECT - 1:
            project_part(c // PROJECT)
    wo_in.wait()

    for t in range(TICKS):
        attend_all(t)
        for q in range(T):
            @pl.when(p == q)
            def _():
                for event in orders[t][q]:
                    step(t, q, *event)
        with jax.named_scope("drain"):
            drain(t)


def store(out, held, out_hbm, held_hbm, out_sem, held_sem):
    copies = (pltpu.make_async_copy(out, out_hbm, out_sem),
              pltpu.make_async_copy(held, held_hbm, held_sem))
    for copy in copies:
        copy.start()
    for copy in copies:
        copy.wait()


def body(acts, fresh, order, ln_gain, ln_bias, wqkv, wo):
    S, T = lax.axis_size("section"), lax.axis_size("tensor")
    slots, tokens, D = acts.shape[1:]
    rows = tokens // CHUNKS
    cols = wqkv.shape[2]
    vmem = pl.BlockSpec(memory_space=pltpu.VMEM)
    hbm = pl.BlockSpec(memory_space=pltpu.HBM)
    block = (TICKS, CHUNKS, rows, D)
    wide = (TICKS, CHUNKS, T, rows, D)
    sem = lambda *shape: pltpu.SemaphoreType.DMA(shape)
    out, held = pl.pallas_call(
        functools.partial(kernel, S, T),
        name="relay",
        out_shape=(jax.ShapeDtypeStruct(block, jnp.bfloat16),) * 2,
        in_specs=[hbm, hbm, hbm, hbm, hbm, hbm, hbm],
        out_specs=(vmem, vmem),
        scratch_shapes=[
            pltpu.SMEM(order.shape, jnp.int32),
            pltpu.VMEM(block, jnp.bfloat16),
            pltpu.VMEM((1, D), jnp.float32),
            pltpu.VMEM((1, D), jnp.float32),
            pltpu.VMEM((D, cols), jnp.bfloat16),
            pltpu.VMEM(wo.shape[1:], jnp.bfloat16),
            pltpu.VMEM(wide, jnp.bfloat16),
            pltpu.VMEM((CHUNKS, T, rows, D), jnp.bfloat16),
            pltpu.VMEM((T * tokens, cols), jnp.bfloat16),
            pltpu.VMEM((ATTEND * T * rows, cols // 3), jnp.bfloat16),
            pltpu.VMEM(wide, jnp.bfloat16),
            pltpu.VMEM(wide, jnp.bfloat16),
            pltpu.VMEM(wide, jnp.bfloat16),
            pltpu.VMEM(block, jnp.bfloat16),
            pltpu.VMEM(block, jnp.bfloat16),
            *[pltpu.SemaphoreType.DMA] * 6,
            sem(TICKS, CHUNKS, T), sem(CHUNKS, T - 1), sem(CHUNKS, T - 1),
            sem(TICKS), sem(TICKS), sem(TICKS, CHUNKS), sem(TICKS),
        ],
        compiler_params=pltpu.CompilerParams(
            collective_id=0, has_side_effects=True, vmem_limit_bytes=32 << 20),
    )(*(pltpu.with_memory_space_constraint(x, pltpu.HBM) for x in (
        order, acts.reshape(slots, CHUNKS, rows, D), fresh.reshape(TICKS, CHUNKS, rows, D),
        ln_gain, ln_bias, wqkv[0], wo[0],
    )))
    out, held = pl.pallas_call(
        store, name="store",
        out_shape=(jax.ShapeDtypeStruct(block, jnp.bfloat16),) * 2,
        in_specs=[vmem, vmem], out_specs=(hbm, hbm),
        scratch_shapes=[pltpu.SemaphoreType.DMA, pltpu.SemaphoreType.DMA],
        compiler_params=pltpu.CompilerParams(vmem_limit_bytes=4 << 20),
    )(out, held)
    return out.reshape(TICKS, 1, tokens, D), held.reshape(1, slots, tokens, D)


def solution(mesh):
    return jax.shard_map(
        body,
        mesh=mesh,
        in_specs=(
            P("section", "dp", "tensor", None),
            P("dp", "tensor", None),
            P("section", None),
            P("section", None),
            P("section", None),
            P("section", None, "tensor"),
            P("section", "tensor", None),
        ),
        out_specs=(P("dp", "section", "tensor", None), P("section", "dp", "tensor", None)),
        check_vma=False,
    )
```

```python
import functools
import math

import jax
import jax.numpy as jnp
from jax import lax
from jax.experimental import pallas as pl
from jax.experimental.pallas import tpu as pltpu
from jax.sharding import PartitionSpec as P

HD = 128
TICKS = 2
CHUNKS = 8
ATTEND = 2
PROJECT = 4
MESH = pl.DeviceIdType.MESH


def plan(T, C, steps, queue):
    last, per = T - 1, C // steps
    wire, reach, hop_wire, hop_reach = 5.64 / C, 2.2, 2.82 / C, 2.6
    add, norm, attend, project = 0.5 / C, 0.8 / C, 1.0, 1.7
    clock, free, arrivals = [0.0] * T, {}, {}

    def send(link, key, at, wire=wire, reach=reach):
        free[link] = max(at, free.get(link, 0.0)) + wire
        arrivals[key] = free[link] + reach

    orders = []
    for t in range(TICKS):
        for p in range(T):
            for k in range(steps):
                clock[p] += attend
                for q, (c, d) in queue(t, k):
                    if p == q:
                        send((p, d > p), ("sum", t, p + 1 if d > p else p - 1, c, d, d > p), clock[p])
        todo, order = [], [[] for _ in range(T)]
        for p in range(T):
            todo.append([("up", c, d) for c in range(C) for d in range(p + 1, T) if p > 0]
                        + [("down", c, d) for c in range(C) for d in range(p) if p < last]
                        + [("own", c, p) for c in range(C)] + [("next", c, p) for c in range(C)])
            if t == 0:
                todo[p] += [("left", c, b) for c in range(C) for b in range(p)]
                todo[p] += [("right", c, b) for c in range(C) for b in range(p + 1, T)]
                todo[p] += [("project", k, p) for k in range(C // PROJECT)]
        sums = ("up", "down", "own")
        rank = {"up": 0, "down": 0, "own": 1, "next": 2, "left": 3, "right": 3, "project": 4}

        def ready(p, kind, c, d):
            need = []
            if kind == "up" or (kind == "own" and p > 0):
                need.append(("sum", t, p, c, d, True))
            if kind == "down" or (kind == "own" and p < last):
                need.append(("sum", t, p, c, d, False))
            if kind == "next":
                need.append(("hop", t, p, c))
                if c == C - 1 and any(e[0] in sums for e in todo[p]):
                    return None
            if kind in ("left", "right"):
                need.append(("gather", p, c, d))
            if kind == "project" and any(
                    e[0] in ("next", "left", "right") and e[1] // PROJECT == c for e in todo[p]):
                return None
            times = [arrivals.get(key) for key in need]
            return None if None in times else max([clock[p]] + times)

        while any(todo):
            at, _, c, p, (kind, c, d) = min(
                (ready(p, *e), rank[e[0]], e[1], p, e)
                for p in range(T) for e in todo[p] if ready(p, *e) is not None)
            todo[p].remove((kind, c, d))
            order[p].append((kind, c, d))
            if kind in ("up", "down"):
                up = kind == "up"
                at += add
                send((p, up), ("sum", t, p + 1 if up else p - 1, c, d, up), at)
            elif kind == "own":
                at += add
                if t == 0:
                    for q in (p - 1, p + 1):
                        if 0 <= q < T:
                            send((p, q > p), ("gather", q, c, p), at, reach=reach + 0.7)
                send((p, "hop"), ("hop", t, p, c), at, hop_wire, hop_reach)
            elif kind == "project":
                at += project
            elif t == 0:
                if kind == "left" and p < last:
                    send((p, True), ("gather", p + 1, c, d), at)
                if kind == "right" and p > 0:
                    send((p, False), ("gather", p - 1, c, d), at)
                at += norm
            clock[p] = at
        orders.append(order)
    return orders


def edge_queue(T, C, steps):
    last, per = T - 1, C // steps
    lead = (0, 5, 7)

    def queue(t, k):
        turns = [(i, c) if t == TICKS - 1 else (c + lead[i], -i, c) for c in range(C) for i in range(last)]
        turns = sorted(zip(turns, [(c, i) for c in range(C) for i in range(last)]))
        at, sends = 0, []
        for _, (c, i) in turns:
            at = max(at, c // per)
            if at == k:
                sends += [(0, (c, last - i)), (last, (c, i))]
        return sends

    return queue


def kernel(
    S, T, order_hbm, acts_hbm, fresh_hbm, gain_hbm, bias_hbm, wq_hbm, wo_hbm, out, held,
    order, acts, gain, bias, wq, wo, xa, norm, qkv, attn, part, from_left, from_right, res, hop,
    mine, other, flag, flag_next, chosen,
    order_sem, acts_sem, gain_sem, bias_sem, wq_sem, wo_sem, ag_first, ag_recv, rl_recv, rr_recv,
    sent_right, sent_left, hop_first, hop_recv, hop_sent, next_sent, back_recv, back_sent,
):
    C = CHUNKS
    rows, D = xa.shape[3], xa.shape[4]
    group = T * rows
    local_heads = qkv.shape[1] // (3 * HD)
    p = lax.axis_index("tensor")
    s = lax.axis_index("section")
    last = T - 1
    steps = C // ATTEND
    queue = edge_queue(T, C, steps)
    orders = plan(T, C, steps, queue)

    barrier = pltpu.get_barrier_semaphore()
    links = ((p > 0, {"tensor": p - 1}), (p < last, {"tensor": p + 1}),
             (s > 0, {"section": s - 1}), (s < S - 1, {"section": s + 1}),
             *(((0 <= q) & (q <= last) & (0 <= r) & (r < S), {"section": r, "tensor": q})
               for q in (p - 1, p + 1) for r in (s - 1, s + 1)))
    for there, device in links:
        @pl.when(there)
        def _():
            pl.semaphore_signal(barrier, inc=1, device_id=device, device_id_type=MESH)

    order_in = pltpu.make_async_copy(order_hbm, order, order_sem)
    acts_in = pltpu.make_async_copy(acts_hbm, acts, acts_sem)
    gain_in = pltpu.make_async_copy(gain_hbm, gain, gain_sem)
    bias_in = pltpu.make_async_copy(bias_hbm, bias, bias_sem)
    wq_in = pltpu.make_async_copy(wq_hbm, wq, wq_sem)
    wo_in = pltpu.make_async_copy(wo_hbm, wo, wo_sem)
    for copy in (order_in, acts_in, gain_in, bias_in, wq_in, wo_in):
        copy.start()

    @pl.when(s == 0)
    def _():
        pltpu.make_async_copy(fresh_hbm.at[0], hop.at[0], hop_first).start()
        for c in range(C):
            pltpu.make_async_copy(fresh_hbm.at[1, c], hop.at[1, c], hop_recv.at[c]).start()

    def scoped(name):
        return lambda f: jax.named_scope(name)(f)

    def gather_copy(t, c, b, right):
        where = pl.ds(2 * c, 2) if t == 0 else c
        return pltpu.make_async_remote_copy(
            src_ref=xa.at[t, where, b], dst_ref=xa.at[t, where, b],
            send_sem=(sent_right if right else sent_left).at[t],
            recv_sem=ag_first.at[c, b] if t == 0 else ag_recv.at[c, b],
            device_id={"tensor": p + 1 if right else p - 1}, device_id_type=MESH)

    def sum_copy(t, c, d, right):
        return pltpu.make_async_remote_copy(
            src_ref=part.at[t, c, d], dst_ref=(from_left if right else from_right).at[t, c, d],
            send_sem=(sent_right if right else sent_left).at[t],
            recv_sem=rl_recv.at[t, c, d - 1] if right else rr_recv.at[t, c, d],
            device_id={"tensor": p + 1 if right else p - 1}, device_id_type=MESH)

    def hop_copy(c):
        return pltpu.make_async_remote_copy(
            src_ref=res.at[1, c], dst_ref=hop.at[1, c],
            send_sem=hop_sent.at[1], recv_sem=hop_recv.at[c],
            device_id={"section": s + 1}, device_id_type=MESH)

    def first_hop():
        return pltpu.make_async_remote_copy(
            src_ref=res.at[0], dst_ref=hop.at[0], send_sem=hop_sent.at[0], recv_sem=hop_first,
            device_id={"section": s + 1}, device_id_type=MESH)

    def next_copy(c, q, side):
        return pltpu.make_async_remote_copy(
            src_ref=chosen.at[c], dst_ref=xa.at[1, c, q],
            send_sem=next_sent.at[side + 1], recv_sem=ag_recv.at[c, q],
            device_id={"section": s + 1, "tensor": q + side}, device_id_type=MESH)

    def back_copies():
        return [pltpu.make_async_remote_copy(
            src_ref=src, dst_ref=dst, send_sem=back_sent.at[i], recv_sem=back_recv.at[i],
            device_id={"section": s - 1}, device_id_type=MESH)
            for i, (src, dst) in enumerate(((flag, flag_next), (mine, other)))]

    @scoped("gather_own")
    def gather_own(t, c):
        @pl.when(p < last)
        def _():
            gather_copy(t, c, p, True).start()

        @pl.when(p > 0)
        def _():
            gather_copy(t, c, p, False).start()

    @scoped("normed")
    def normed(t, c, b):
        values = xa[t, c, b].astype(jnp.float32)
        centred = values - jnp.mean(values, axis=-1, keepdims=True)
        spread = jnp.mean(centred * centred, axis=-1, keepdims=True)
        norm[c, b] = (
            centred * lax.rsqrt(spread + 1e-06) * gain[...] + bias[...]
        ).astype(jnp.bfloat16)

    @scoped("gather_step")
    def gather_step(c, j):
        b_left, b_right = p - 1 - j, p + 1 + j

        @pl.when(b_left >= 0)
        def _():
            copy = gather_copy(0, c, b_left, True)
            copy.wait_recv()

            @pl.when(p < last)
            def _():
                copy.start()

        @pl.when(b_right <= last)
        def _():
            copy = gather_copy(0, c, b_right, False)
            copy.wait_recv()

            @pl.when(p > 0)
            def _():
                copy.start()

        for there, b in ((b_left >= 0, b_left), (b_right <= last, b_right)):
            @pl.when(there)
            def _():
                normed(0, 2 * c, b)
                normed(0, 2 * c + 1, b)

    @scoped("project")
    def project(part_of, begin, width):
        span = PROJECT * group

        @pl.loop(0, local_heads)
        def _(h):
            cols = pl.ds(pl.multiple_of(h * (3 * HD), HD) + begin, width)
            qkv[part_of * span:(part_of + 1) * span, cols] = jnp.dot(
                norm[PROJECT * part_of:PROJECT * (part_of + 1)].reshape(span, D), wq[:, cols],
                preferred_element_type=jnp.float32,
            ).astype(jnp.bfloat16)

    def project_keys(part_of):
        project(part_of, HD, 2 * HD)

    def project_queries(part_of):
        project(part_of, 0, HD)

    def project_part(part_of):
        project_keys(part_of)
        if part_of < C // PROJECT - 1:
            project_queries(part_of)

    def attend_all(t):
        half = steps // (C // PROJECT)

        for part in range(C // PROJECT):
            @pl.loop(part * half, (part + 1) * half)
            def _(k):
                attend(t, k)

            if part == C // PROJECT - 2:
                project_queries(part + 1)

    @scoped("attend")
    def attend(t, part_of):
        span = ATTEND * group
        r0 = pl.multiple_of(part_of * span, span)
        heads = range(local_heads)

        def columns(h, j):
            return slice((h * 3 + j) * HD, (h * 3 + j + 1) * HD)

        scores = [lax.dot_general(
            qkv[pl.ds(r0, span), columns(h, 0)], qkv[:, columns(h, 1)],
            (((1,), (1,)), ((), ())), preferred_element_type=jnp.float32) for h in heads]
        scores = [x * (1.0 / math.sqrt(HD)) for x in scores]
        tops = [jnp.max(x, axis=-1, keepdims=True) for x in scores]
        powers = [jnp.exp(x - top) for x, top in zip(scores, tops)]
        sums = [jnp.sum(x, axis=-1, keepdims=True) for x in powers]
        probs = [(x * (1.0 / total)).astype(jnp.bfloat16) for x, total in zip(powers, sums)]
        mixed = [jnp.dot(probs[h], qkv[:, columns(h, 2)], preferred_element_type=jnp.float32)
                 for h in heads]
        for h in heads:
            attn[:, h * HD:(h + 1) * HD] = mixed[h].astype(jnp.bfloat16)
        width = min(512, D)
        for n in range(D // width):
            cols = slice(n * width, (n + 1) * width)
            block = jnp.dot(attn[...], wo[:, cols], preferred_element_type=jnp.float32)
            block = block.reshape(ATTEND, T, rows, width).astype(jnp.bfloat16)
            part[t, pl.ds(part_of * ATTEND, ATTEND), :, :, cols] = block
        for k in range(steps):
            for q in (0, last):
                @pl.when((part_of == k) & (p == q))
                def _():
                    for end, (c, d) in queue(t, k):
                        if end == q:
                            sum_copy(t, c, d, q == 0).start()

    def pass_sum(t, c, d, right):
        copy = sum_copy(t, c, d, right)
        copy.wait_recv()
        came = from_left if right else from_right
        part[t, c, d] = (
            part[t, c, d].astype(jnp.float32) + came[t, c, d].astype(jnp.float32)
        ).astype(jnp.bfloat16)
        copy.start()

    @scoped("sum_own")
    def sum_own(t, c, q):
        total = part[t, c, q].astype(jnp.float32)
        if q > 0:
            sum_copy(t, c, q, True).wait_recv()
            total += from_left[t, c, q].astype(jnp.float32)
        if q < last:
            sum_copy(t, c, q, False).wait_recv()
            total += from_right[t, c, q].astype(jnp.float32)
        result = (xa[t, c, q].astype(jnp.float32) + total).astype(jnp.bfloat16)
        res[t, c] = result

        @pl.when(s < S - 1)
        def _():
            if t == 0:
                chosen[c] = jnp.where(flag_next[0:1, 0:1] > 0.5, result.astype(jnp.float32),
                                      other[c].astype(jnp.float32)).astype(jnp.bfloat16)
                for side in (1, -1, 0):
                    if 0 <= q + side <= last:
                        next_copy(c, q, side).start()
            else:
                hop_copy(c).start()
        out[t, c] = result

    @scoped("arrived")
    def arrived(c):
        pltpu.make_async_copy(fresh_hbm.at[1, c], hop.at[1, c], hop_recv.at[c]).wait()

    def sent_all(src, sem):
        pltpu.make_async_remote_copy(
            src_ref=src, dst_ref=src, send_sem=sem, recv_sem=hop_first,
            device_id={"section": s + 1}, device_id_type=MESH).wait_send()

    def drain(t):
        for there, sem in ((p < last, sent_right), (p > 0, sent_left)):
            @pl.when(there)
            def _():
                if t == 0:
                    sent_all(xa.at[0], sem.at[0])
                else:
                    sent_all(xa.at[1, :, pl.ds(0, last)], sem.at[1])

                    @pl.when(s == 0)
                    def _():
                        sent_all(res.at[1], sem.at[1])

        @pl.when(s < S - 1)
        def _():
            sent_all(res.at[t], hop_sent.at[t])
            if t == 0:
                sent_all(chosen, next_sent.at[1])

                @pl.when(p > 0)
                def _():
                    sent_all(chosen, next_sent.at[0])

                @pl.when(p < last)
                def _():
                    sent_all(chosen, next_sent.at[2])

        if t == 0:
            @pl.when(s > 0)
            def _():
                for copy in back_copies():
                    copy.wait_send()

    def step(t, q, kind, c, d):
        if kind in ("up", "down"):
            with jax.named_scope("pass_sum"):
                pass_sum(t, c, d, kind == "up")
        elif kind == "own":
            sum_own(t, c, q)
        elif kind == "project":
            project_part(c)
        elif kind == "next" and t == 0:
            @pl.when(s == 0)
            def _():
                xa[1, c, q] = jnp.where(first == second, hop[0, c], acts[second, c])
                if q < last:
                    gather_copy(1, c, q, True).start()
                if q > 0:
                    gather_copy(1, c, q, False).start()

            @pl.when(s > 0)
            def _():
                gather_copy(1, c, q, q < last).wait_recv()
            normed(1, c, q)
        elif kind == "next":
            arrived(c)
            for j in range(2):
                held[j, c] = jnp.where(
                    second == j, hop[1, c], jnp.where(first == j, hop[0, c], acts[j, c]))
        else:
            with jax.named_scope("gather_step"):
                copy = gather_copy(1, c, d, kind == "left")
                copy.wait_recv()
                if (q < last) if kind == "left" else (q > 0):
                    copy.start()
            normed(1, c, d)

    with jax.named_scope("acts_wait"):
        order_in.wait()
        acts_in.wait()
    first, second = order[0, 0], order[0, 1]
    for c in range(C):
        xa[0, c, p] = acts[first, c]
    with jax.named_scope("entry"):
        pl.semaphore_wait(barrier, sum(there.astype(jnp.int32) for there, _ in links))
    for c in range(C // 2):
        gather_own(0, c)

    @pl.when(s > 0)
    def _():
        for c in range(C):
            mine[c] = acts[second, c]
        flag[...] = jnp.full(flag.shape, jnp.where(first == second, 1.0, 0.0), jnp.float32)
        for copy in back_copies():
            copy.start()
    gain_in.wait()
    bias_in.wait()
    for c in range(C):
        normed(0, c, p)
    for j in range(last - 1):
        for c in range(C // 2):
            gather_step(c, j)
    wq_in.wait()
    for c in range(C // 2):
        gather_step(c, last - 1)
        if (2 * c + 1) % PROJECT == PROJECT - 1:
            project_part(2 * c // PROJECT)
    wo_in.wait()

    for t in range(TICKS):
        attend_all(t)
        if t == 0:
            @pl.when(s < S - 1)
            def _():
                for copy in back_copies():
                    copy.wait_recv()

            @pl.when(s == 0)
            def _():
                pltpu.make_async_copy(fresh_hbm.at[0], hop.at[0], hop_first).wait()
        for q in range(T):
            @pl.when(p == q)
            def _():
                owns, nexts = 0, 0
                for event in orders[t][q]:
                    if t == 1 and event[0] == "next":
                        if nexts == 0:
                            @pl.when(s > 0)
                            def _():
                                first_hop().wait_recv()
                        nexts += 1
                    step(t, q, *event)
                    if t == 0 and event[0] == "own":
                        owns += 1
                        if owns == C:
                            @pl.when(s < S - 1)
                            def _():
                                first_hop().start()
        with jax.named_scope("drain"):
            drain(t)


def store(out, held, out_hbm, held_hbm, out_sem, held_sem):
    copies = (pltpu.make_async_copy(out, out_hbm, out_sem),
              pltpu.make_async_copy(held, held_hbm, held_sem))
    for copy in copies:
        copy.start()
    for copy in copies:
        copy.wait()


def body(acts, fresh, order, ln_gain, ln_bias, wqkv, wo):
    S, T = lax.axis_size("section"), lax.axis_size("tensor")
    slots, tokens, D = acts.shape[1:]
    rows = tokens // CHUNKS
    cols = wqkv.shape[2]
    vmem = pl.BlockSpec(memory_space=pltpu.VMEM)
    hbm = pl.BlockSpec(memory_space=pltpu.HBM)
    block = (TICKS, CHUNKS, rows, D)
    wide = (TICKS, CHUNKS, T, rows, D)
    sem = lambda *shape: pltpu.SemaphoreType.DMA(shape)
    out, held = pl.pallas_call(
        functools.partial(kernel, S, T),
        name="relay",
        out_shape=(jax.ShapeDtypeStruct(block, jnp.bfloat16),) * 2,
        in_specs=[hbm, hbm, hbm, hbm, hbm, hbm, hbm],
        out_specs=(vmem, vmem),
        scratch_shapes=[
            pltpu.SMEM(order.shape, jnp.int32),
            pltpu.VMEM(block, jnp.bfloat16),
            pltpu.VMEM((1, D), jnp.float32),
            pltpu.VMEM((1, D), jnp.float32),
            pltpu.VMEM((D, cols), jnp.bfloat16),
            pltpu.VMEM(wo.shape[1:], jnp.bfloat16),
            pltpu.VMEM(wide, jnp.bfloat16),
            pltpu.VMEM((CHUNKS, T, rows, D), jnp.bfloat16),
            pltpu.VMEM((T * tokens, cols), jnp.bfloat16),
            pltpu.VMEM((ATTEND * T * rows, cols // 3), jnp.bfloat16),
            pltpu.VMEM(wide, jnp.bfloat16),
            pltpu.VMEM(wide, jnp.bfloat16),
            pltpu.VMEM(wide, jnp.bfloat16),
            pltpu.VMEM(block, jnp.bfloat16),
            pltpu.VMEM(block, jnp.bfloat16),
            pltpu.VMEM(block[1:], jnp.bfloat16),
            pltpu.VMEM(block[1:], jnp.bfloat16),
            pltpu.VMEM((8, 128), jnp.float32),
            pltpu.VMEM((8, 128), jnp.float32),
            pltpu.VMEM(block[1:], jnp.bfloat16),
            *[pltpu.SemaphoreType.DMA] * 6,
            sem(CHUNKS // 2, T), sem(CHUNKS, T), sem(TICKS, CHUNKS, T - 1), sem(TICKS, CHUNKS, T - 1),
            sem(TICKS), sem(TICKS), pltpu.SemaphoreType.DMA, sem(CHUNKS), sem(TICKS), sem(3), sem(2), sem(2),
        ],
        compiler_params=pltpu.CompilerParams(
            collective_id=0, has_side_effects=True, vmem_limit_bytes=32 << 20),
    )(*(pltpu.with_memory_space_constraint(x, pltpu.HBM) for x in (
        order, acts.reshape(slots, CHUNKS, rows, D), fresh.reshape(TICKS, CHUNKS, rows, D),
        ln_gain, ln_bias, wqkv[0], wo[0],
    )))
    out, held = pl.pallas_call(
        store, name="store",
        out_shape=(jax.ShapeDtypeStruct(block, jnp.bfloat16),) * 2,
        in_specs=[vmem, vmem], out_specs=(hbm, hbm),
        scratch_shapes=[pltpu.SemaphoreType.DMA, pltpu.SemaphoreType.DMA],
        compiler_params=pltpu.CompilerParams(vmem_limit_bytes=4 << 20),
    )(out, held)
    return out.reshape(TICKS, 1, tokens, D), held.reshape(1, slots, tokens, D)


def solution(mesh):
    return jax.shard_map(
        body,
        mesh=mesh,
        in_specs=(
            P("section", "dp", "tensor", None),
            P("dp", "tensor", None),
            P("section", None),
            P("section", None),
            P("section", None),
            P("section", None, "tensor"),
            P("section", "tensor", None),
        ),
        out_specs=(P("dp", "section", "tensor", None), P("section", "dp", "tensor", None)),
        check_vma=False,
    )
```

```python
import functools
import math

import jax
import jax.numpy as jnp
from jax import lax
from jax.experimental import pallas as pl
from jax.experimental.pallas import tpu as pltpu
from jax.sharding import PartitionSpec as P

HD = 128
TICKS = 2
CHUNKS = 8
ATTEND = 2
PROJECT = 4
MESH = pl.DeviceIdType.MESH


def plan(T, C, steps, queue):
    last, per = T - 1, C // steps
    wire, reach, hop_wire, hop_reach = 5.64 / C, 2.2, 2.82 / C, 2.6
    add, norm, attend, project = 0.8 / C, 1.6 / C, 1.0, 2.0
    clock, free, arrivals = [0.0] * T, {}, {}

    def send(link, key, at, wire=wire, reach=reach):
        free[link] = max(at, free.get(link, 0.0)) + wire
        arrivals[key] = free[link] + reach

    orders = []
    for t in range(TICKS):
        for p in range(T):
            for k in range(steps):
                clock[p] += attend
                for q, (c, d) in queue(t, k):
                    if p == q:
                        send((p, d > p), ("sum", t, p + 1 if d > p else p - 1, c, d, d > p), clock[p])
        todo, order = [], [[] for _ in range(T)]
        for p in range(T):
            todo.append([("up", c, d) for c in range(C) for d in range(p + 1, T) if p > 0]
                        + [("down", c, d) for c in range(C) for d in range(p) if p < last]
                        + [("own", c, p) for c in range(C)] + [("next", c, p) for c in range(C)])
            if t == 0:
                todo[p] += [("left", c, b) for c in range(C) for b in range(p)]
                todo[p] += [("right", c, b) for c in range(C) for b in range(p + 1, T)]
                todo[p] += [("project", k, p) for k in range(C // PROJECT)]
        sums = ("up", "down", "own")
        rank = {"up": 0, "down": 0, "own": 1, "next": 2, "left": 3, "right": 3, "project": 4}

        def ready(p, kind, c, d):
            need = []
            if kind == "up" or (kind == "own" and p > 0):
                need.append(("sum", t, p, c, d, True))
            if kind == "down" or (kind == "own" and p < last):
                need.append(("sum", t, p, c, d, False))
            if kind == "next":
                need.append(("hop", t, p, c))
                if c == C - 1 and any(e[0] in sums for e in todo[p]):
                    return None
            if kind in ("left", "right"):
                need.append(("gather", p, c, d))
            if kind == "project" and any(
                    e[0] in ("next", "left", "right") and (e[1] // PROJECT == c or 0 < p < last)
                    for e in todo[p]):
                return None
            times = [arrivals.get(key) for key in need]
            return None if None in times else max([clock[p]] + times)

        while any(todo):
            at, _, c, p, (kind, c, d) = min(
                (ready(p, *e), rank[e[0]], e[1], p, e)
                for p in range(T) for e in todo[p] if ready(p, *e) is not None)
            todo[p].remove((kind, c, d))
            order[p].append((kind, c, d))
            if kind in ("up", "down"):
                up = kind == "up"
                at += add
                send((p, up), ("sum", t, p + 1 if up else p - 1, c, d, up), at)
            elif kind == "own":
                at += add
                send((p, "hop"), ("hop", t, p, c), at, hop_wire, hop_reach)
            elif kind == "project":
                at += project
            elif t == 0:
                if kind in ("next", "left") and p < last:
                    send((p, True), ("gather", p + 1, c, d), at)
                if kind in ("next", "right") and p > 0:
                    send((p, False), ("gather", p - 1, c, d), at)
                at += norm if p in (0, last) else 0.02
            clock[p] = at
        orders.append(order)
    return orders


def edge_queue(T, C, steps):
    last, per = T - 1, C // steps
    lead = (0, 5, 7)

    def queue(t, k):
        turns = [(i, c) if t == TICKS - 1 else (c + lead[i], -i, c) for c in range(C) for i in range(last)]
        turns = sorted(zip(turns, [(c, i) for c in range(C) for i in range(last)]))
        at, sends = 0, []
        for _, (c, i) in turns:
            at = max(at, c // per)
            if at == k:
                sends += [(0, (c, last - i)), (last, (c, i))]
        return sends

    return queue


def kernel(
    S, T, order_hbm, acts_hbm, fresh_hbm, gain_hbm, bias_hbm, wq_hbm, wo_hbm, out, held,
    order, acts, gain, bias, wq, wo, xa, norm, qkv, attn, part, from_left, from_right, res, hop,
    order_sem, acts_sem, gain_sem, bias_sem, wq_sem, wo_sem, ag_recv, rl_recv, rr_recv,
    sent_right, sent_left, hop_recv, hop_sent,
):
    C = CHUNKS
    rows, D = xa.shape[3], xa.shape[4]
    group = T * rows
    local_heads = qkv.shape[1] // (3 * HD)
    p = lax.axis_index("tensor")
    s = lax.axis_index("section")
    last = T - 1
    steps = C // ATTEND
    queue = edge_queue(T, C, steps)
    orders = plan(T, C, steps, queue)

    barrier = pltpu.get_barrier_semaphore()
    links = ((p > 0, {"tensor": p - 1}), (p < last, {"tensor": p + 1}),
             (s > 0, {"section": s - 1}), (s < S - 1, {"section": s + 1}))
    for there, device in links:
        @pl.when(there)
        def _():
            pl.semaphore_signal(barrier, inc=1, device_id=device, device_id_type=MESH)

    order_in = pltpu.make_async_copy(order_hbm, order, order_sem)
    acts_in = pltpu.make_async_copy(acts_hbm, acts, acts_sem)
    gain_in = pltpu.make_async_copy(gain_hbm, gain, gain_sem)
    bias_in = pltpu.make_async_copy(bias_hbm, bias, bias_sem)
    wq_in = pltpu.make_async_copy(wq_hbm, wq, wq_sem)
    wo_in = pltpu.make_async_copy(wo_hbm, wo, wo_sem)
    for copy in (order_in, acts_in, gain_in, bias_in, wq_in, wo_in):
        copy.start()

    @pl.when(s == 0)
    def _():
        for t in range(TICKS):
            for c in range(C):
                pltpu.make_async_copy(fresh_hbm.at[t, c], hop.at[t, c], hop_recv.at[t, c]).start()

    def scoped(name):
        return lambda f: jax.named_scope(name)(f)

    def gather_copy(t, c, b, right):
        return pltpu.make_async_remote_copy(
            src_ref=xa.at[t, c, b], dst_ref=xa.at[t, c, b],
            send_sem=(sent_right if right else sent_left).at[t], recv_sem=ag_recv.at[t, c, b],
            device_id={"tensor": p + 1 if right else p - 1}, device_id_type=MESH)

    def sum_copy(t, c, d, right):
        return pltpu.make_async_remote_copy(
            src_ref=part.at[t, c, d], dst_ref=(from_left if right else from_right).at[t, c, d],
            send_sem=(sent_right if right else sent_left).at[t],
            recv_sem=rl_recv.at[c, d - 1] if right else rr_recv.at[c, d],
            device_id={"tensor": p + 1 if right else p - 1}, device_id_type=MESH)

    def hop_copy(t, c):
        return pltpu.make_async_remote_copy(
            src_ref=res.at[t, c], dst_ref=hop.at[t, c],
            send_sem=hop_sent.at[t], recv_sem=hop_recv.at[t, c],
            device_id={"section": s + 1}, device_id_type=MESH)

    @scoped("gather_own")
    def gather_own(t, c):
        @pl.when(p < last)
        def _():
            gather_copy(t, c, p, True).start()

        @pl.when(p > 0)
        def _():
            gather_copy(t, c, p, False).start()

    @scoped("normed")
    def normed(t, c, b):
        values = xa[t, c, b].astype(jnp.float32)
        centred = values - jnp.mean(values, axis=-1, keepdims=True)
        spread = jnp.mean(centred * centred, axis=-1, keepdims=True)
        norm[c, b] = (
            centred * lax.rsqrt(spread + 1e-06) * gain[...] + bias[...]
        ).astype(jnp.bfloat16)

    @scoped("normed")
    def normed_chunks(t, begin):
        @pl.loop(begin, begin + PROJECT)
        def _(c):
            values = xa[t, c].astype(jnp.float32).reshape(group, D)
            centred = values - jnp.mean(values, axis=-1, keepdims=True)
            spread = jnp.mean(centred * centred, axis=-1, keepdims=True)
            scaled = centred * lax.rsqrt(spread + 1e-06) * gain[...] + bias[...]
            norm[c] = scaled.reshape(T, rows, D).astype(jnp.bfloat16)

    @scoped("gather_step")
    def gather_step(t, c, j):
        b_left, b_right = p - 1 - j, p + 1 + j

        @pl.when(b_left >= 0)
        def _():
            copy = gather_copy(t, c, b_left, True)
            copy.wait_recv()

            @pl.when(p < last)
            def _():
                copy.start()

        @pl.when(b_right <= last)
        def _():
            copy = gather_copy(t, c, b_right, False)
            copy.wait_recv()

            @pl.when(p > 0)
            def _():
                copy.start()

        @pl.when(b_left >= 0)
        def _():
            normed(t, c, b_left)

        @pl.when(b_right <= last)
        def _():
            normed(t, c, b_right)

    def project(part_of, columns):
        span = PROJECT * group
        weights = [wq[:, cols] for cols in columns]
        result = jnp.dot(
            norm[PROJECT * part_of:PROJECT * (part_of + 1)].reshape(span, D),
            weights[0] if len(weights) == 1 else jnp.concatenate(weights, axis=1),
            preferred_element_type=jnp.float32,
        ).astype(jnp.bfloat16)
        at = 0
        for cols in columns:
            qkv[part_of * span:(part_of + 1) * span, cols] = result[:, at:at + cols.size]
            at += cols.size

    def head_columns(h, begin, width):
        return pl.ds(pl.multiple_of(h * (3 * HD), HD) + begin, width)

    @scoped("project")
    def project_keys(part_of):
        @pl.loop(0, local_heads)
        def _(h):
            project(part_of, [head_columns(h, HD, 2 * HD)])

    @scoped("project")
    def project_queries(part_of):
        pair = math.gcd(2, local_heads)

        @pl.loop(0, local_heads // pair)
        def _(h):
            project(part_of, [head_columns(pair * h + i, 0, HD) for i in range(pair)])

    def project_part(part_of):
        project_keys(part_of)
        if part_of < C // PROJECT - 1:
            project_queries(part_of)

    def attend_all(t):
        half = steps // (C // PROJECT)

        for part in range(C // PROJECT):
            @pl.loop(part * half, (part + 1) * half)
            def _(k):
                attend(t, k)

            if part == C // PROJECT - 2:
                project_queries(part + 1)

    @scoped("attend")
    def attend(t, part_of):
        span = ATTEND * group
        r0 = pl.multiple_of(part_of * span, span)
        heads = range(local_heads)

        def columns(h, j):
            return slice((h * 3 + j) * HD, (h * 3 + j + 1) * HD)

        scores = [lax.dot_general(
            qkv[pl.ds(r0, span), columns(h, 0)], qkv[:, columns(h, 1)],
            (((1,), (1,)), ((), ())), preferred_element_type=jnp.float32) for h in heads]
        scores = [x * (1.0 / math.sqrt(HD)) for x in scores]
        tops = [jnp.max(x, axis=-1, keepdims=True) for x in scores]
        powers = [jnp.exp(x - top) for x, top in zip(scores, tops)]
        sums = [jnp.sum(x, axis=-1, keepdims=True) for x in powers]
        probs = [(x * (1.0 / total)).astype(jnp.bfloat16) for x, total in zip(powers, sums)]
        mixed = [jnp.dot(probs[h], qkv[:, columns(h, 2)], preferred_element_type=jnp.float32)
                 for h in heads]
        for h in heads:
            attn[:, h * HD:(h + 1) * HD] = mixed[h].astype(jnp.bfloat16)
        width = min(512, D)
        for n in range(D // width):
            cols = slice(n * width, (n + 1) * width)
            block = jnp.dot(attn[...], wo[:, cols], preferred_element_type=jnp.float32)
            block = block.reshape(ATTEND, T, rows, width).astype(jnp.bfloat16)
            part[t, pl.ds(part_of * ATTEND, ATTEND), :, :, cols] = block
        for k in range(steps):
            for q in (0, last):
                @pl.when((part_of == k) & (p == q))
                def _():
                    for end, (c, d) in queue(t, k):
                        if end == q:
                            sum_copy(t, c, d, q == 0).start()

    def pass_sum(t, c, d, right):
        copy = sum_copy(t, c, d, right)
        copy.wait_recv()
        came = from_left if right else from_right
        part[t, c, d] = (
            part[t, c, d].astype(jnp.float32) + came[t, c, d].astype(jnp.float32)
        ).astype(jnp.bfloat16)
        copy.start()

    @scoped("sum_own")
    def sum_own(t, c, q):
        total = part[t, c, q].astype(jnp.float32)
        if q > 0:
            sum_copy(t, c, q, True).wait_recv()
            total += from_left[t, c, q].astype(jnp.float32)
        if q < last:
            sum_copy(t, c, q, False).wait_recv()
            total += from_right[t, c, q].astype(jnp.float32)
        result = (xa[t, c, q].astype(jnp.float32) + total).astype(jnp.bfloat16)
        res[t, c] = result

        @pl.when(s < S - 1)
        def _():
            hop_copy(t, c).start()
        out[t, c] = result

    @scoped("arrived")
    def arrived(t, c):
        pltpu.make_async_copy(fresh_hbm.at[t, c], hop.at[t, c], hop_recv.at[t, c]).wait()

    def drain(t):
        for right, there in ((True, p < last), (False, p > 0)):
            @pl.when(there)
            def _():
                pltpu.make_async_remote_copy(
                    src_ref=xa.at[t], dst_ref=xa.at[t],
                    send_sem=(sent_right if right else sent_left).at[t], recv_sem=ag_recv.at[t, 0, 0],
                    device_id={"tensor": p + 1 if right else p - 1}, device_id_type=MESH,
                ).wait_send()

        @pl.when(s < S - 1)
        def _():
            pltpu.make_async_remote_copy(
                src_ref=res.at[t], dst_ref=hop.at[t],
                send_sem=hop_sent.at[t], recv_sem=hop_recv.at[t, 0],
                device_id={"section": s + 1}, device_id_type=MESH).wait_send()

    def step(t, q, kind, c, d):
        if kind in ("up", "down"):
            with jax.named_scope("pass_sum"):
                pass_sum(t, c, d, kind == "up")
        elif kind == "own":
            sum_own(t, c, q)
        elif kind == "project":
            if 0 < q < last:
                normed_chunks(1, c * PROJECT)
            project_part(c)
        elif kind == "next" and t == 0:
            arrived(0, c)
            xa[1, c, q] = jnp.where(first == second, hop[0, c], acts[second, c])
            if q < last:
                gather_copy(1, c, q, True).start()
            if q > 0:
                gather_copy(1, c, q, False).start()
            if q in (0, last):
                normed(1, c, q)
        elif kind == "next":
            arrived(1, c)
            for j in range(2):
                held[j, c] = jnp.where(
                    second == j, hop[1, c], jnp.where(first == j, hop[0, c], acts[j, c]))
        else:
            with jax.named_scope("gather_step"):
                copy = gather_copy(1, c, d, kind == "left")
                copy.wait_recv()
                if (q < last) if kind == "left" else (q > 0):
                    copy.start()
            if q in (0, last):
                normed(1, c, d)

    with jax.named_scope("acts_wait"):
        order_in.wait()
        acts_in.wait()
    first, second = order[0, 0], order[0, 1]
    for c in range(C):
        xa[0, c, p] = acts[first, c]
    with jax.named_scope("entry"):
        pl.semaphore_wait(barrier, sum(there.astype(jnp.int32) for there, _ in links))
    for c in range(C):
        gather_own(0, c)

    gain_in.wait()
    bias_in.wait()
    for c in range(C):
        normed(0, c, p)
    for j in range(last - 1):
        for c in range(C):
            gather_step(0, c, j)
    wq_in.wait()
    for c in range(C):
        gather_step(0, c, last - 1)
        if c % PROJECT == PROJECT - 1:
            project_part(c // PROJECT)
    wo_in.wait()

    for t in range(TICKS):
        attend_all(t)
        for q in range(T):
            @pl.when(p == q)
            def _():
                for event in orders[t][q]:
                    step(t, q, *event)
        with jax.named_scope("drain"):
            drain(t)


def store(out, held, out_hbm, held_hbm, out_sem, held_sem):
    copies = (pltpu.make_async_copy(out, out_hbm, out_sem),
              pltpu.make_async_copy(held, held_hbm, held_sem))
    for copy in copies:
        copy.start()
    for copy in copies:
        copy.wait()


def body(acts, fresh, order, ln_gain, ln_bias, wqkv, wo):
    S, T = lax.axis_size("section"), lax.axis_size("tensor")
    slots, tokens, D = acts.shape[1:]
    rows = tokens // CHUNKS
    cols = wqkv.shape[2]
    vmem = pl.BlockSpec(memory_space=pltpu.VMEM)
    hbm = pl.BlockSpec(memory_space=pltpu.HBM)
    block = (TICKS, CHUNKS, rows, D)
    wide = (TICKS, CHUNKS, T, rows, D)
    sem = lambda *shape: pltpu.SemaphoreType.DMA(shape)
    out, held = pl.pallas_call(
        functools.partial(kernel, S, T),
        name="relay",
        out_shape=(jax.ShapeDtypeStruct(block, jnp.bfloat16),) * 2,
        in_specs=[hbm, hbm, hbm, hbm, hbm, hbm, hbm],
        out_specs=(vmem, vmem),
        scratch_shapes=[
            pltpu.SMEM(order.shape, jnp.int32),
            pltpu.VMEM(block, jnp.bfloat16),
            pltpu.VMEM((1, D), jnp.float32),
            pltpu.VMEM((1, D), jnp.float32),
            pltpu.VMEM((D, cols), jnp.bfloat16),
            pltpu.VMEM(wo.shape[1:], jnp.bfloat16),
            pltpu.VMEM(wide, jnp.bfloat16),
            pltpu.VMEM((CHUNKS, T, rows, D), jnp.bfloat16),
            pltpu.VMEM((T * tokens, cols), jnp.bfloat16),
            pltpu.VMEM((ATTEND * T * rows, cols // 3), jnp.bfloat16),
            pltpu.VMEM(wide, jnp.bfloat16),
            pltpu.VMEM(wide, jnp.bfloat16),
            pltpu.VMEM(wide, jnp.bfloat16),
            pltpu.VMEM(block, jnp.bfloat16),
            pltpu.VMEM(block, jnp.bfloat16),
            *[pltpu.SemaphoreType.DMA] * 6,
            sem(TICKS, CHUNKS, T), sem(CHUNKS, T - 1), sem(CHUNKS, T - 1),
            sem(TICKS), sem(TICKS), sem(TICKS, CHUNKS), sem(TICKS),
        ],
        compiler_params=pltpu.CompilerParams(
            collective_id=0, has_side_effects=True, vmem_limit_bytes=32 << 20),
    )(*(pltpu.with_memory_space_constraint(x, pltpu.HBM) for x in (
        order, acts.reshape(slots, CHUNKS, rows, D), fresh.reshape(TICKS, CHUNKS, rows, D),
        ln_gain, ln_bias, wqkv[0], wo[0],
    )))
    out, held = pl.pallas_call(
        store, name="store",
        out_shape=(jax.ShapeDtypeStruct(block, jnp.bfloat16),) * 2,
        in_specs=[vmem, vmem], out_specs=(hbm, hbm),
        scratch_shapes=[pltpu.SemaphoreType.DMA, pltpu.SemaphoreType.DMA],
        compiler_params=pltpu.CompilerParams(vmem_limit_bytes=4 << 20),
    )(out, held)
    return out.reshape(TICKS, 1, tokens, D), held.reshape(1, slots, tokens, D)


def solution(mesh):
    return jax.shard_map(
        body,
        mesh=mesh,
        in_specs=(
            P("section", "dp", "tensor", None),
            P("dp", "tensor", None),
            P("section", None),
            P("section", None),
            P("section", None),
            P("section", None, "tensor"),
            P("section", "tensor", None),
        ),
        out_specs=(P("dp", "section", "tensor", None), P("section", "dp", "tensor", None)),
        check_vma=False,
    )
```

```python
import functools
import math

import jax
import jax.numpy as jnp
from jax import lax
from jax.experimental import pallas as pl
from jax.experimental.pallas import tpu as pltpu
from jax.sharding import PartitionSpec as P

HD = 128
TICKS = 2
CHUNKS = 8
ATTEND = 2
PROJECT = 4
MESH = pl.DeviceIdType.MESH


def plan(T, C, steps, queue):
    last, per = T - 1, C // steps
    wire, reach, hop_wire, hop_reach = 5.64 / C, 2.2, 2.82 / C, 2.6
    add, norm, attend, project = 0.8 / C, 1.6 / C, 1.0, 2.0
    clock, free, arrivals = [0.0] * T, {}, {}

    def send(link, key, at, wire=wire, reach=reach):
        free[link] = max(at, free.get(link, 0.0)) + wire
        arrivals[key] = free[link] + reach

    orders = []
    for t in range(TICKS):
        for p in range(T):
            for k in range(steps):
                clock[p] += attend
                for q, (c, d) in queue(t, k):
                    if p == q:
                        send((p, d > p), ("sum", t, p + 1 if d > p else p - 1, c, d, d > p), clock[p])
        todo, order = [], [[] for _ in range(T)]
        for p in range(T):
            todo.append([("up", c, d) for c in range(C) for d in range(p + 1, T) if p > 0]
                        + [("down", c, d) for c in range(C) for d in range(p) if p < last]
                        + [("own", c, p) for c in range(C)] + [("next", c, p) for c in range(C)])
            if t == 0:
                todo[p] += [("left", c, b) for c in range(C) for b in range(p)]
                todo[p] += [("right", c, b) for c in range(C) for b in range(p + 1, T)]
                todo[p] += [("project", k, p) for k in range(C // PROJECT)]
        sums = ("up", "down", "own")
        rank = {"up": 0, "down": 0, "own": 1, "next": 2, "left": 3, "right": 3, "project": 4}

        def ready(p, kind, c, d):
            need = []
            if kind == "up" or (kind == "own" and p > 0):
                need.append(("sum", t, p, c, d, True))
            if kind == "down" or (kind == "own" and p < last):
                need.append(("sum", t, p, c, d, False))
            if kind == "next":
                need.append(("hop", t, p, c))
                if c == C - 1 and any(e[0] in sums for e in todo[p]):
                    return None
            if kind in ("left", "right"):
                need.append(("gather", p, c, d))
            if kind == "project" and any(
                    e[0] in ("next", "left", "right") and (e[1] // PROJECT == c or 0 < p < last)
                    for e in todo[p]):
                return None
            times = [arrivals.get(key) for key in need]
            return None if None in times else max([clock[p]] + times)

        while any(todo):
            at, _, c, p, (kind, c, d) = min(
                (ready(p, *e), rank[e[0]], e[1], p, e)
                for p in range(T) for e in todo[p] if ready(p, *e) is not None)
            todo[p].remove((kind, c, d))
            order[p].append((kind, c, d))
            if kind in ("up", "down"):
                up = kind == "up"
                at += add
                send((p, up), ("sum", t, p + 1 if up else p - 1, c, d, up), at)
            elif kind == "own":
                at += add
                send((p, "hop"), ("hop", t, p, c), at, hop_wire, hop_reach)
            elif kind == "project":
                at += project
            elif t == 0:
                if kind in ("next", "left") and p < last:
                    send((p, True), ("gather", p + 1, c, d), at)
                if kind in ("next", "right") and p > 0:
                    send((p, False), ("gather", p - 1, c, d), at)
                at += norm if p in (0, last) else 0.02
            clock[p] = at
        orders.append(order)
    return orders


def edge_queue(T, C, steps):
    last, per = T - 1, C // steps
    lead = (0, 5, 7)

    def queue(t, k):
        turns = [(i, c) if t == TICKS - 1 else (c + lead[i], -i, c) for c in range(C) for i in range(last)]
        turns = sorted(zip(turns, [(c, i) for c in range(C) for i in range(last)]))
        at, sends = 0, []
        for _, (c, i) in turns:
            at = max(at, c // per)
            if at == k:
                sends += [(0, (c, last - i)), (last, (c, i))]
        return sends

    return queue


def kernel(
    S, T, order_hbm, acts_hbm, fresh_hbm, gain_hbm, bias_hbm, wq_hbm, wo_hbm, out, held,
    order, acts, gain, bias, wq, wo, xa, norm, qkv, attn, part, from_left, from_right, res, hop,
    order_sem, acts_sem, gain_sem, bias_sem, wq_sem, wo_sem, ag_recv, rl_recv, rr_recv,
    sent_right, sent_left, hop_recv, hop_sent,
):
    C = CHUNKS
    rows, D = xa.shape[3], xa.shape[4]
    group = T * rows
    local_heads = qkv.shape[1] // (3 * HD)
    p = lax.axis_index("tensor")
    s = lax.axis_index("section")
    last = T - 1
    steps = C // ATTEND
    queue = edge_queue(T, C, steps)
    orders = plan(T, C, steps, queue)

    barrier = pltpu.get_barrier_semaphore()
    links = ((p > 0, {"tensor": p - 1}), (p < last, {"tensor": p + 1}),
             (s > 0, {"section": s - 1}), (s < S - 1, {"section": s + 1}))
    for there, device in links:
        @pl.when(there)
        def _():
            pl.semaphore_signal(barrier, inc=1, device_id=device, device_id_type=MESH)

    order_in = pltpu.make_async_copy(order_hbm, order, order_sem)
    acts_in = pltpu.make_async_copy(acts_hbm, acts, acts_sem)
    gain_in = pltpu.make_async_copy(gain_hbm, gain, gain_sem)
    bias_in = pltpu.make_async_copy(bias_hbm, bias, bias_sem)
    wq_in = pltpu.make_async_copy(wq_hbm, wq, wq_sem)
    wo_in = pltpu.make_async_copy(wo_hbm, wo, wo_sem)
    for copy in (order_in, acts_in, gain_in, bias_in, wq_in, wo_in):
        copy.start()

    @pl.when(s == 0)
    def _():
        for t in range(TICKS):
            for c in range(C):
                pltpu.make_async_copy(fresh_hbm.at[t, c], hop.at[t, c], hop_recv.at[t, c]).start()

    def scoped(name):
        return lambda f: jax.named_scope(name)(f)

    def gather_copy(t, c, b, right):
        return pltpu.make_async_remote_copy(
            src_ref=xa.at[t, c, b], dst_ref=xa.at[t, c, b],
            send_sem=(sent_right if right else sent_left).at[t], recv_sem=ag_recv.at[t, c, b],
            device_id={"tensor": p + 1 if right else p - 1}, device_id_type=MESH)

    def sum_copy(t, c, d, right):
        return pltpu.make_async_remote_copy(
            src_ref=part.at[t, c, d], dst_ref=(from_left if right else from_right).at[t, c, d],
            send_sem=(sent_right if right else sent_left).at[t],
            recv_sem=rl_recv.at[c, d - 1] if right else rr_recv.at[c, d],
            device_id={"tensor": p + 1 if right else p - 1}, device_id_type=MESH)

    def hop_copy(t, c):
        return pltpu.make_async_remote_copy(
            src_ref=res.at[t, c], dst_ref=hop.at[t, c],
            send_sem=hop_sent.at[t], recv_sem=hop_recv.at[t, c],
            device_id={"section": s + 1}, device_id_type=MESH)

    @scoped("gather_own")
    def gather_own(t, c):
        @pl.when(p < last)
        def _():
            gather_copy(t, c, p, True).start()

        @pl.when(p > 0)
        def _():
            gather_copy(t, c, p, False).start()

    @scoped("normed")
    def normed(t, c, b):
        values = xa[t, c, b].astype(jnp.float32)
        centred = values - jnp.mean(values, axis=-1, keepdims=True)
        spread = jnp.mean(centred * centred, axis=-1, keepdims=True)
        norm[c, b] = (
            centred * lax.rsqrt(spread + 1e-06) * gain[...] + bias[...]
        ).astype(jnp.bfloat16)

    @scoped("normed")
    def normed_chunks(t, begin):
        @pl.loop(begin, begin + PROJECT)
        def _(c):
            values = xa[t, c].astype(jnp.float32).reshape(group, D)
            centred = values - jnp.mean(values, axis=-1, keepdims=True)
            spread = jnp.mean(centred * centred, axis=-1, keepdims=True)
            scaled = centred * lax.rsqrt(spread + 1e-06) * gain[...] + bias[...]
            norm[c] = scaled.reshape(T, rows, D).astype(jnp.bfloat16)

    @scoped("gather_step")
    def gather_step(t, c, j):
        def forward(b, there, right):
            @pl.when(there)
            def _():
                copy = gather_copy(t, c, b, right)
                copy.wait_recv()

                @pl.when((p < last) if right else (p > 0))
                def _():
                    copy.start()

                @pl.when((p == 0) | (p == last))
                def _():
                    normed(t, c, b)

        b_left, b_right = p - 1 - j, p + 1 + j
        forward(b_right, (b_right <= last) & (p < T // 2), False)
        forward(b_left, b_left >= 0, True)
        forward(b_right, (b_right <= last) & (p >= T // 2), False)

    def project(part_of, columns):
        span = PROJECT * group
        weights = [wq[:, cols] for cols in columns]
        result = jnp.dot(
            norm[PROJECT * part_of:PROJECT * (part_of + 1)].reshape(span, D),
            weights[0] if len(weights) == 1 else jnp.concatenate(weights, axis=1),
            preferred_element_type=jnp.float32,
        ).astype(jnp.bfloat16)
        at = 0
        for cols in columns:
            qkv[part_of * span:(part_of + 1) * span, cols] = result[:, at:at + cols.size]
            at += cols.size

    def head_columns(h, begin, width):
        return pl.ds(pl.multiple_of(h * (3 * HD), HD) + begin, width)

    @scoped("project")
    def project_keys(part_of):
        @pl.loop(0, local_heads)
        def _(h):
            project(part_of, [head_columns(h, HD, 2 * HD)])

    @scoped("project")
    def project_queries(part_of):
        pair = math.gcd(2, local_heads)

        @pl.loop(0, local_heads // pair)
        def _(h):
            project(part_of, [head_columns(pair * h + i, 0, HD) for i in range(pair)])

    def project_part(part_of):
        project_keys(part_of)
        if part_of < C // PROJECT - 1:
            project_queries(part_of)

    def attend_all(t):
        half = steps // (C // PROJECT)

        for part in range(C // PROJECT):
            @pl.loop(part * half, (part + 1) * half)
            def _(k):
                attend(t, k)

            if part == C // PROJECT - 2:
                project_queries(part + 1)

    @scoped("attend")
    def attend(t, part_of):
        span = ATTEND * group
        r0 = pl.multiple_of(part_of * span, span)
        heads = range(local_heads)

        def columns(h, j):
            return slice((h * 3 + j) * HD, (h * 3 + j + 1) * HD)

        scores = [lax.dot_general(
            qkv[pl.ds(r0, span), columns(h, 0)], qkv[:, columns(h, 1)],
            (((1,), (1,)), ((), ())), preferred_element_type=jnp.float32) for h in heads]
        scores = [x * (1.0 / math.sqrt(HD)) for x in scores]
        tops = [jnp.max(x, axis=-1, keepdims=True) for x in scores]
        powers = [jnp.exp(x - top) for x, top in zip(scores, tops)]
        sums = [jnp.sum(x, axis=-1, keepdims=True) for x in powers]
        probs = [(x * (1.0 / total)).astype(jnp.bfloat16) for x, total in zip(powers, sums)]
        mixed = [jnp.dot(probs[h], qkv[:, columns(h, 2)], preferred_element_type=jnp.float32)
                 for h in heads]
        for h in heads:
            attn[:, h * HD:(h + 1) * HD] = mixed[h].astype(jnp.bfloat16)
        width = min(512, D)
        for n in range(D // width):
            cols = slice(n * width, (n + 1) * width)
            block = jnp.dot(attn[...], wo[:, cols], preferred_element_type=jnp.float32)
            block = block.reshape(ATTEND, T, rows, width).astype(jnp.bfloat16)
            part[t, pl.ds(part_of * ATTEND, ATTEND), :, :, cols] = block
        for k in range(steps):
            for q in (0, last):
                @pl.when((part_of == k) & (p == q))
                def _():
                    for end, (c, d) in queue(t, k):
                        if end == q:
                            sum_copy(t, c, d, q == 0).start()

    def pass_sum(t, c, d, right):
        copy = sum_copy(t, c, d, right)
        copy.wait_recv()
        came = from_left if right else from_right
        part[t, c, d] = (
            part[t, c, d].astype(jnp.float32) + came[t, c, d].astype(jnp.float32)
        ).astype(jnp.bfloat16)
        copy.start()

    @scoped("sum_own")
    def sum_own(t, c, q):
        total = part[t, c, q].astype(jnp.float32)
        if q > 0:
            sum_copy(t, c, q, True).wait_recv()
            total += from_left[t, c, q].astype(jnp.float32)
        if q < last:
            sum_copy(t, c, q, False).wait_recv()
            total += from_right[t, c, q].astype(jnp.float32)
        result = (xa[t, c, q].astype(jnp.float32) + total).astype(jnp.bfloat16)
        res[t, c] = result

        @pl.when(s < S - 1)
        def _():
            hop_copy(t, c).start()
        out[t, c] = result

    @scoped("arrived")
    def arrived(t, c):
        pltpu.make_async_copy(fresh_hbm.at[t, c], hop.at[t, c], hop_recv.at[t, c]).wait()

    def drain(t):
        for right, there in ((True, p < last), (False, p > 0)):
            @pl.when(there)
            def _():
                pltpu.make_async_remote_copy(
                    src_ref=xa.at[t], dst_ref=xa.at[t],
                    send_sem=(sent_right if right else sent_left).at[t], recv_sem=ag_recv.at[t, 0, 0],
                    device_id={"tensor": p + 1 if right else p - 1}, device_id_type=MESH,
                ).wait_send()

        @pl.when(s < S - 1)
        def _():
            pltpu.make_async_remote_copy(
                src_ref=res.at[t], dst_ref=hop.at[t],
                send_sem=hop_sent.at[t], recv_sem=hop_recv.at[t, 0],
                device_id={"section": s + 1}, device_id_type=MESH).wait_send()

    def step(t, q, kind, c, d):
        if kind in ("up", "down"):
            with jax.named_scope("pass_sum"):
                pass_sum(t, c, d, kind == "up")
        elif kind == "own":
            sum_own(t, c, q)
        elif kind == "project":
            if 0 < q < last:
                normed_chunks(1, c * PROJECT)
            project_part(c)
        elif kind == "next" and t == 0:
            arrived(0, c)
            xa[1, c, q] = jnp.where(first == second, hop[0, c], acts[second, c])
            if q < last:
                gather_copy(1, c, q, True).start()
            if q > 0:
                gather_copy(1, c, q, False).start()
            if q in (0, last):
                normed(1, c, q)
        elif kind == "next":
            arrived(1, c)
            for j in range(2):
                held[j, c] = jnp.where(
                    second == j, hop[1, c], jnp.where(first == j, hop[0, c], acts[j, c]))
        else:
            with jax.named_scope("gather_step"):
                copy = gather_copy(1, c, d, kind == "left")
                copy.wait_recv()
                if (q < last) if kind == "left" else (q > 0):
                    copy.start()
            if q in (0, last):
                normed(1, c, d)

    with jax.named_scope("acts_wait"):
        order_in.wait()
        acts_in.wait()
    first, second = order[0, 0], order[0, 1]
    for c in range(C):
        xa[0, c, p] = acts[first, c]
    with jax.named_scope("entry"):
        pl.semaphore_wait(barrier, sum(there.astype(jnp.int32) for there, _ in links))
    for c in range(C):
        gather_own(0, c)

    gain_in.wait()
    bias_in.wait()
    edge = (p == 0) | (p == last)

    @pl.when(edge)
    def _():
        for c in range(C):
            normed(0, c, p)
    for j in range(last - 1):
        for c in range(C):
            gather_step(0, c, j)
    wq_in.wait()
    for c in range(C):
        gather_step(0, c, last - 1)
        if c % PROJECT == PROJECT - 1:
            @pl.when(~edge)
            def _():
                normed_chunks(0, c + 1 - PROJECT)
            project_part(c // PROJECT)
    wo_in.wait()

    for t in range(TICKS):
        attend_all(t)
        for q in range(T):
            @pl.when(p == q)
            def _():
                for event in orders[t][q]:
                    step(t, q, *event)
        with jax.named_scope("drain"):
            drain(t)


def store(out, held, out_hbm, held_hbm, out_sem, held_sem):
    copies = (pltpu.make_async_copy(out, out_hbm, out_sem),
              pltpu.make_async_copy(held, held_hbm, held_sem))
    for copy in copies:
        copy.start()
    for copy in copies:
        copy.wait()


def body(acts, fresh, order, ln_gain, ln_bias, wqkv, wo):
    S, T = lax.axis_size("section"), lax.axis_size("tensor")
    slots, tokens, D = acts.shape[1:]
    rows = tokens // CHUNKS
    cols = wqkv.shape[2]
    vmem = pl.BlockSpec(memory_space=pltpu.VMEM)
    hbm = pl.BlockSpec(memory_space=pltpu.HBM)
    block = (TICKS, CHUNKS, rows, D)
    wide = (TICKS, CHUNKS, T, rows, D)
    sem = lambda *shape: pltpu.SemaphoreType.DMA(shape)
    out, held = pl.pallas_call(
        functools.partial(kernel, S, T),
        name="relay",
        out_shape=(jax.ShapeDtypeStruct(block, jnp.bfloat16),) * 2,
        in_specs=[hbm, hbm, hbm, hbm, hbm, hbm, hbm],
        out_specs=(vmem, vmem),
        scratch_shapes=[
            pltpu.SMEM(order.shape, jnp.int32),
            pltpu.VMEM(block, jnp.bfloat16),
            pltpu.VMEM((1, D), jnp.float32),
            pltpu.VMEM((1, D), jnp.float32),
            pltpu.VMEM((D, cols), jnp.bfloat16),
            pltpu.VMEM(wo.shape[1:], jnp.bfloat16),
            pltpu.VMEM(wide, jnp.bfloat16),
            pltpu.VMEM((CHUNKS, T, rows, D), jnp.bfloat16),
            pltpu.VMEM((T * tokens, cols), jnp.bfloat16),
            pltpu.VMEM((ATTEND * T * rows, cols // 3), jnp.bfloat16),
            pltpu.VMEM(wide, jnp.bfloat16),
            pltpu.VMEM(wide, jnp.bfloat16),
            pltpu.VMEM(wide, jnp.bfloat16),
            pltpu.VMEM(block, jnp.bfloat16),
            pltpu.VMEM(block, jnp.bfloat16),
            *[pltpu.SemaphoreType.DMA] * 6,
            sem(TICKS, CHUNKS, T), sem(CHUNKS, T - 1), sem(CHUNKS, T - 1),
            sem(TICKS), sem(TICKS), sem(TICKS, CHUNKS), sem(TICKS),
        ],
        compiler_params=pltpu.CompilerParams(
            collective_id=0, has_side_effects=True, vmem_limit_bytes=32 << 20),
    )(*(pltpu.with_memory_space_constraint(x, pltpu.HBM) for x in (
        order, acts.reshape(slots, CHUNKS, rows, D), fresh.reshape(TICKS, CHUNKS, rows, D),
        ln_gain, ln_bias, wqkv[0], wo[0],
    )))
    out, held = pl.pallas_call(
        store, name="store",
        out_shape=(jax.ShapeDtypeStruct(block, jnp.bfloat16),) * 2,
        in_specs=[vmem, vmem], out_specs=(hbm, hbm),
        scratch_shapes=[pltpu.SemaphoreType.DMA, pltpu.SemaphoreType.DMA],
        compiler_params=pltpu.CompilerParams(vmem_limit_bytes=4 << 20),
    )(out, held)
    return out.reshape(TICKS, 1, tokens, D), held.reshape(1, slots, tokens, D)


def solution(mesh):
    return jax.shard_map(
        body,
        mesh=mesh,
        in_specs=(
            P("section", "dp", "tensor", None),
            P("dp", "tensor", None),
            P("section", None),
            P("section", None),
            P("section", None),
            P("section", None, "tensor"),
            P("section", "tensor", None),
        ),
        out_specs=(P("dp", "section", "tensor", None), P("section", "dp", "tensor", None)),
        check_vma=False,
    )
```

```python
import functools
import math

import jax
import jax.numpy as jnp
from jax import lax
from jax.experimental import pallas as pl
from jax.experimental.pallas import tpu as pltpu
from jax.sharding import PartitionSpec as P

HD = 128
TICKS = 2
CHUNKS = 8
ATTEND = 2
PROJECT = 4
MESH = pl.DeviceIdType.MESH


def plan(T, C, steps, queue):
    last, per = T - 1, C // steps
    wire, reach, hop_wire, hop_reach = 5.64 / C, 2.2, 2.82 / C, 2.6
    add, norm, attend, project = 0.8 / C, 1.6 / C, 1.0, 2.0
    clock, free, arrivals = [0.0] * T, {}, {}

    def send(link, key, at, wire=wire, reach=reach):
        free[link] = max(at, free.get(link, 0.0)) + wire
        arrivals[key] = free[link] + reach

    orders = []
    for t in range(TICKS):
        for p in range(T):
            for k in range(steps):
                clock[p] += attend
                for q, (c, d) in queue(t, k):
                    if p == q:
                        send((p, d > p), ("sum", t, p + 1 if d > p else p - 1, c, d, d > p), clock[p])
        todo, order = [], [[] for _ in range(T)]
        for p in range(T):
            todo.append([("up", c, d) for c in range(C) for d in range(p + 1, T) if p > 0]
                        + [("down", c, d) for c in range(C) for d in range(p) if p < last]
                        + [("own", c, p) for c in range(C)] + [("next", c, p) for c in range(C)])
            if t == 0:
                todo[p] += [("left", c, b) for c in range(C) for b in range(p)]
                todo[p] += [("right", c, b) for c in range(C) for b in range(p + 1, T)]
                todo[p] += [("project", k, p) for k in range(C // PROJECT)]
        sums = ("up", "down", "own")
        rank = {"up": 0, "down": 0, "own": 1, "next": 2, "left": 3, "right": 3, "project": 4}

        def ready(p, kind, c, d):
            need = []
            if kind == "up" or (kind == "own" and p > 0):
                need.append(("sum", t, p, c, d, True))
            if kind == "down" or (kind == "own" and p < last):
                need.append(("sum", t, p, c, d, False))
            if kind == "next":
                need.append(("hop", t, p, c))
                if c == C - 1 and any(e[0] in sums for e in todo[p]):
                    return None
            if kind in ("left", "right"):
                need.append(("gather", p, c, d))
            if kind == "project" and any(
                    e[0] in ("next", "left", "right") and (e[1] // PROJECT == c or 0 < p < last)
                    for e in todo[p]):
                return None
            times = [arrivals.get(key) for key in need]
            return None if None in times else max([clock[p]] + times)

        while any(todo):
            at, _, c, p, (kind, c, d) = min(
                (ready(p, *e), rank[e[0]], e[1], p, e)
                for p in range(T) for e in todo[p] if ready(p, *e) is not None)
            todo[p].remove((kind, c, d))
            order[p].append((kind, c, d))
            if kind in ("up", "down"):
                up = kind == "up"
                at += add
                send((p, up), ("sum", t, p + 1 if up else p - 1, c, d, up), at)
            elif kind == "own":
                at += add
                send((p, "hop"), ("hop", t, p, c), at, hop_wire, hop_reach)
            elif kind == "project":
                at += project
            elif t == 0:
                if kind in ("next", "left") and p < last:
                    send((p, True), ("gather", p + 1, c, d), at)
                if kind in ("next", "right") and p > 0:
                    send((p, False), ("gather", p - 1, c, d), at)
                at += norm if p in (0, last) else 0.02
            clock[p] = at
        orders.append(order)
    return orders


def edge_queue(T, C, steps):
    last, per = T - 1, C // steps
    lead = (0, 5, 7)

    def queue(t, k):
        turns = [(i, c) if t == TICKS - 1 else (c + lead[i], -i, c) for c in range(C) for i in range(last)]
        turns = sorted(zip(turns, [(c, i) for c in range(C) for i in range(last)]))
        at, sends = 0, []
        for _, (c, i) in turns:
            at = max(at, c // per)
            if at == k:
                sends += [(0, (c, last - i)), (last, (c, i))]
        return sends

    return queue


def kernel(
    S, T, order_hbm, acts_hbm, fresh_hbm, gain_hbm, bias_hbm, wq_hbm, wo_hbm, out, held,
    order, acts, gain, bias, wq, wo, xa, norm, qkv, attn, part, from_left, from_right, res, hop,
    order_sem, acts_sem, gain_sem, bias_sem, wq_sem, wo_sem, ag_first, ag_recv, rl_recv, rr_recv,
    sent_right, sent_left, hop_recv, hop_sent,
):
    C = CHUNKS
    rows, D = xa.shape[3], xa.shape[4]
    group = T * rows
    local_heads = qkv.shape[1] // (3 * HD)
    p = lax.axis_index("tensor")
    s = lax.axis_index("section")
    last = T - 1
    steps = C // ATTEND
    queue = edge_queue(T, C, steps)
    orders = plan(T, C, steps, queue)

    barrier = pltpu.get_barrier_semaphore()
    links = ((p > 0, {"tensor": p - 1}), (p < last, {"tensor": p + 1}),
             (s > 0, {"section": s - 1}), (s < S - 1, {"section": s + 1}))
    for there, device in links:
        @pl.when(there)
        def _():
            pl.semaphore_signal(barrier, inc=1, device_id=device, device_id_type=MESH)

    order_in = pltpu.make_async_copy(order_hbm, order, order_sem)
    acts_in = pltpu.make_async_copy(acts_hbm, acts, acts_sem)
    gain_in = pltpu.make_async_copy(gain_hbm, gain, gain_sem)
    bias_in = pltpu.make_async_copy(bias_hbm, bias, bias_sem)
    wq_in = pltpu.make_async_copy(wq_hbm, wq, wq_sem)
    wo_in = pltpu.make_async_copy(wo_hbm, wo, wo_sem)
    for copy in (order_in, acts_in, gain_in, bias_in, wq_in, wo_in):
        copy.start()

    @pl.when(s == 0)
    def _():
        for t in range(TICKS):
            for c in range(C):
                pltpu.make_async_copy(fresh_hbm.at[t, c], hop.at[t, c], hop_recv.at[t, c]).start()

    def scoped(name):
        return lambda f: jax.named_scope(name)(f)

    def gather_copy(t, c, b, right):
        where = pl.ds(2 * c, 2) if t == 0 else c
        return pltpu.make_async_remote_copy(
            src_ref=xa.at[t, where, b], dst_ref=xa.at[t, where, b],
            send_sem=(sent_right if right else sent_left).at[t],
            recv_sem=ag_first.at[c, b] if t == 0 else ag_recv.at[c, b],
            device_id={"tensor": p + 1 if right else p - 1}, device_id_type=MESH)

    def sum_copy(t, c, d, right):
        return pltpu.make_async_remote_copy(
            src_ref=part.at[t, c, d], dst_ref=(from_left if right else from_right).at[t, c, d],
            send_sem=(sent_right if right else sent_left).at[t],
            recv_sem=rl_recv.at[c, d - 1] if right else rr_recv.at[c, d],
            device_id={"tensor": p + 1 if right else p - 1}, device_id_type=MESH)

    def hop_copy(t, c):
        return pltpu.make_async_remote_copy(
            src_ref=res.at[t, c], dst_ref=hop.at[t, c],
            send_sem=hop_sent.at[t], recv_sem=hop_recv.at[t, c],
            device_id={"section": s + 1}, device_id_type=MESH)

    @scoped("gather_own")
    def gather_own(t, c):
        @pl.when(p < last)
        def _():
            gather_copy(t, c, p, True).start()

        @pl.when(p > 0)
        def _():
            gather_copy(t, c, p, False).start()

    @scoped("normed")
    def normed(t, c, b):
        values = xa[t, c, b].astype(jnp.float32)
        centred = values - jnp.mean(values, axis=-1, keepdims=True)
        spread = jnp.mean(centred * centred, axis=-1, keepdims=True)
        norm[c, b] = (
            centred * lax.rsqrt(spread + 1e-06) * gain[...] + bias[...]
        ).astype(jnp.bfloat16)

    @scoped("normed")
    def normed_chunks(t, begin):
        @pl.loop(begin, begin + PROJECT)
        def _(c):
            values = xa[t, c].astype(jnp.float32).reshape(group, D)
            centred = values - jnp.mean(values, axis=-1, keepdims=True)
            spread = jnp.mean(centred * centred, axis=-1, keepdims=True)
            scaled = centred * lax.rsqrt(spread + 1e-06) * gain[...] + bias[...]
            norm[c] = scaled.reshape(T, rows, D).astype(jnp.bfloat16)

    @scoped("gather_step")
    def gather_step(t, c, j):
        def forward(b, there, right):
            @pl.when(there)
            def _():
                copy = gather_copy(t, c, b, right)
                copy.wait_recv()

                @pl.when((p < last) if right else (p > 0))
                def _():
                    copy.start()

                @pl.when((p == 0) | (p == last))
                def _():
                    normed(t, 2 * c, b)
                    normed(t, 2 * c + 1, b)

        b_left, b_right = p - 1 - j, p + 1 + j
        forward(b_right, (b_right <= last) & (p < T // 2), False)
        forward(b_left, b_left >= 0, True)
        forward(b_right, (b_right <= last) & (p >= T // 2), False)

    def project(part_of, columns):
        span = PROJECT * group
        weights = [wq[:, cols] for cols in columns]
        result = jnp.dot(
            norm[PROJECT * part_of:PROJECT * (part_of + 1)].reshape(span, D),
            weights[0] if len(weights) == 1 else jnp.concatenate(weights, axis=1),
            preferred_element_type=jnp.float32,
        ).astype(jnp.bfloat16)
        at = 0
        for cols in columns:
            qkv[part_of * span:(part_of + 1) * span, cols] = result[:, at:at + cols.size]
            at += cols.size

    def head_columns(h, begin, width):
        return pl.ds(pl.multiple_of(h * (3 * HD), HD) + begin, width)

    @scoped("project")
    def project_keys(part_of):
        @pl.loop(0, local_heads)
        def _(h):
            project(part_of, [head_columns(h, HD, 2 * HD)])

    @scoped("project")
    def project_queries(part_of):
        pair = math.gcd(2, local_heads)

        @pl.loop(0, local_heads // pair)
        def _(h):
            project(part_of, [head_columns(pair * h + i, 0, HD) for i in range(pair)])

    def project_part(part_of):
        project_keys(part_of)
        if part_of < C // PROJECT - 1:
            project_queries(part_of)

    def attend_all(t):
        half = steps // (C // PROJECT)

        for part in range(C // PROJECT):
            @pl.loop(part * half, (part + 1) * half)
            def _(k):
                attend(t, k)

            if part == C // PROJECT - 2:
                project_queries(part + 1)

    @scoped("attend")
    def attend(t, part_of):
        span = ATTEND * group
        r0 = pl.multiple_of(part_of * span, span)
        heads = range(local_heads)

        def columns(h, j):
            return slice((h * 3 + j) * HD, (h * 3 + j + 1) * HD)

        scores = [lax.dot_general(
            qkv[pl.ds(r0, span), columns(h, 0)], qkv[:, columns(h, 1)],
            (((1,), (1,)), ((), ())), preferred_element_type=jnp.float32) for h in heads]
        scores = [x * (1.0 / math.sqrt(HD)) for x in scores]
        tops = [jnp.max(x, axis=-1, keepdims=True) for x in scores]
        powers = [jnp.exp(x - top) for x, top in zip(scores, tops)]
        sums = [jnp.sum(x, axis=-1, keepdims=True) for x in powers]
        probs = [(x * (1.0 / total)).astype(jnp.bfloat16) for x, total in zip(powers, sums)]
        mixed = [jnp.dot(probs[h], qkv[:, columns(h, 2)], preferred_element_type=jnp.float32)
                 for h in heads]
        for h in heads:
            attn[:, h * HD:(h + 1) * HD] = mixed[h].astype(jnp.bfloat16)
        width = min(512, D)
        for n in range(D // width):
            cols = slice(n * width, (n + 1) * width)
            block = jnp.dot(attn[...], wo[:, cols], preferred_element_type=jnp.float32)
            block = block.reshape(ATTEND, T, rows, width).astype(jnp.bfloat16)
            part[t, pl.ds(part_of * ATTEND, ATTEND), :, :, cols] = block
        for k in range(steps):
            for q in (0, last):
                @pl.when((part_of == k) & (p == q))
                def _():
                    for end, (c, d) in queue(t, k):
                        if end == q:
                            sum_copy(t, c, d, q == 0).start()

    def pass_sum(t, c, d, right):
        copy = sum_copy(t, c, d, right)
        copy.wait_recv()
        came = from_left if right else from_right
        part[t, c, d] = (
            part[t, c, d].astype(jnp.float32) + came[t, c, d].astype(jnp.float32)
        ).astype(jnp.bfloat16)
        copy.start()

    @scoped("sum_own")
    def sum_own(t, c, q):
        total = part[t, c, q].astype(jnp.float32)
        if q > 0:
            sum_copy(t, c, q, True).wait_recv()
            total += from_left[t, c, q].astype(jnp.float32)
        if q < last:
            sum_copy(t, c, q, False).wait_recv()
            total += from_right[t, c, q].astype(jnp.float32)
        result = (xa[t, c, q].astype(jnp.float32) + total).astype(jnp.bfloat16)
        res[t, c] = result

        @pl.when(s < S - 1)
        def _():
            hop_copy(t, c).start()
        out[t, c] = result

    @scoped("arrived")
    def arrived(t, c):
        pltpu.make_async_copy(fresh_hbm.at[t, c], hop.at[t, c], hop_recv.at[t, c]).wait()

    def drain(t):
        for right, there in ((True, p < last), (False, p > 0)):
            @pl.when(there)
            def _():
                pltpu.make_async_remote_copy(
                    src_ref=xa.at[t], dst_ref=xa.at[t],
                    send_sem=(sent_right if right else sent_left).at[t], recv_sem=ag_recv.at[0, 0],
                    device_id={"tensor": p + 1 if right else p - 1}, device_id_type=MESH,
                ).wait_send()

        @pl.when(s < S - 1)
        def _():
            pltpu.make_async_remote_copy(
                src_ref=res.at[t], dst_ref=hop.at[t],
                send_sem=hop_sent.at[t], recv_sem=hop_recv.at[t, 0],
                device_id={"section": s + 1}, device_id_type=MESH).wait_send()

    def step(t, q, kind, c, d):
        if kind in ("up", "down"):
            with jax.named_scope("pass_sum"):
                pass_sum(t, c, d, kind == "up")
        elif kind == "own":
            sum_own(t, c, q)
        elif kind == "project":
            if 0 < q < last:
                normed_chunks(1, c * PROJECT)
            project_part(c)
        elif kind == "next" and t == 0:
            arrived(0, c)
            xa[1, c, q] = jnp.where(first == second, hop[0, c], acts[second, c])
            if q < last:
                gather_copy(1, c, q, True).start()
            if q > 0:
                gather_copy(1, c, q, False).start()
            if q in (0, last):
                normed(1, c, q)
        elif kind == "next":
            arrived(1, c)
            for j in range(2):
                held[j, c] = jnp.where(
                    second == j, hop[1, c], jnp.where(first == j, hop[0, c], acts[j, c]))
        else:
            with jax.named_scope("gather_step"):
                copy = gather_copy(1, c, d, kind == "left")
                copy.wait_recv()
                if (q < last) if kind == "left" else (q > 0):
                    copy.start()
            if q in (0, last):
                normed(1, c, d)

    with jax.named_scope("acts_wait"):
        order_in.wait()
        acts_in.wait()
    first, second = order[0, 0], order[0, 1]
    for c in range(C):
        xa[0, c, p] = acts[first, c]
    with jax.named_scope("entry"):
        pl.semaphore_wait(barrier, sum(there.astype(jnp.int32) for there, _ in links))
    for c in range(C // 2):
        gather_own(0, c)

    gain_in.wait()
    bias_in.wait()
    edge = (p == 0) | (p == last)

    @pl.when(edge)
    def _():
        for c in range(C):
            normed(0, c, p)
    for j in range(last - 1):
        for c in range(C // 2):
            gather_step(0, c, j)
    wq_in.wait()
    for c in range(1, C, 2):
        gather_step(0, c // 2, last - 1)
        if c % PROJECT == PROJECT - 1:
            @pl.when(~edge)
            def _():
                normed_chunks(0, c + 1 - PROJECT)
            project_part(c // PROJECT)
    wo_in.wait()

    for t in range(TICKS):
        attend_all(t)
        for q in range(T):
            @pl.when(p == q)
            def _():
                for event in orders[t][q]:
                    step(t, q, *event)
        with jax.named_scope("drain"):
            drain(t)


def store(out, held, out_hbm, held_hbm, out_sem, held_sem):
    copies = (pltpu.make_async_copy(out, out_hbm, out_sem),
              pltpu.make_async_copy(held, held_hbm, held_sem))
    for copy in copies:
        copy.start()
    for copy in copies:
        copy.wait()


def body(acts, fresh, order, ln_gain, ln_bias, wqkv, wo):
    S, T = lax.axis_size("section"), lax.axis_size("tensor")
    slots, tokens, D = acts.shape[1:]
    rows = tokens // CHUNKS
    cols = wqkv.shape[2]
    vmem = pl.BlockSpec(memory_space=pltpu.VMEM)
    hbm = pl.BlockSpec(memory_space=pltpu.HBM)
    block = (TICKS, CHUNKS, rows, D)
    wide = (TICKS, CHUNKS, T, rows, D)
    sem = lambda *shape: pltpu.SemaphoreType.DMA(shape)
    out, held = pl.pallas_call(
        functools.partial(kernel, S, T),
        name="relay",
        out_shape=(jax.ShapeDtypeStruct(block, jnp.bfloat16),) * 2,
        in_specs=[hbm, hbm, hbm, hbm, hbm, hbm, hbm],
        out_specs=(vmem, vmem),
        scratch_shapes=[
            pltpu.SMEM(order.shape, jnp.int32),
            pltpu.VMEM(block, jnp.bfloat16),
            pltpu.VMEM((1, D), jnp.float32),
            pltpu.VMEM((1, D), jnp.float32),
            pltpu.VMEM((D, cols), jnp.bfloat16),
            pltpu.VMEM(wo.shape[1:], jnp.bfloat16),
            pltpu.VMEM(wide, jnp.bfloat16),
            pltpu.VMEM((CHUNKS, T, rows, D), jnp.bfloat16),
            pltpu.VMEM((T * tokens, cols), jnp.bfloat16),
            pltpu.VMEM((ATTEND * T * rows, cols // 3), jnp.bfloat16),
            pltpu.VMEM(wide, jnp.bfloat16),
            pltpu.VMEM(wide, jnp.bfloat16),
            pltpu.VMEM(wide, jnp.bfloat16),
            pltpu.VMEM(block, jnp.bfloat16),
            pltpu.VMEM(block, jnp.bfloat16),
            *[pltpu.SemaphoreType.DMA] * 6,
            sem(CHUNKS // 2, T), sem(CHUNKS, T), sem(CHUNKS, T - 1), sem(CHUNKS, T - 1),
            sem(TICKS), sem(TICKS), sem(TICKS, CHUNKS), sem(TICKS),
        ],
        compiler_params=pltpu.CompilerParams(
            collective_id=0, has_side_effects=True, vmem_limit_bytes=32 << 20),
    )(*(pltpu.with_memory_space_constraint(x, pltpu.HBM) for x in (
        order, acts.reshape(slots, CHUNKS, rows, D), fresh.reshape(TICKS, CHUNKS, rows, D),
        ln_gain, ln_bias, wqkv[0], wo[0],
    )))
    out, held = pl.pallas_call(
        store, name="store",
        out_shape=(jax.ShapeDtypeStruct(block, jnp.bfloat16),) * 2,
        in_specs=[vmem, vmem], out_specs=(hbm, hbm),
        scratch_shapes=[pltpu.SemaphoreType.DMA, pltpu.SemaphoreType.DMA],
        compiler_params=pltpu.CompilerParams(vmem_limit_bytes=4 << 20),
    )(out, held)
    return out.reshape(TICKS, 1, tokens, D), held.reshape(1, slots, tokens, D)


def solution(mesh):
    return jax.shard_map(
        body,
        mesh=mesh,
        in_specs=(
            P("section", "dp", "tensor", None),
            P("dp", "tensor", None),
            P("section", None),
            P("section", None),
            P("section", None),
            P("section", None, "tensor"),
            P("section", "tensor", None),
        ),
        out_specs=(P("dp", "section", "tensor", None), P("section", "dp", "tensor", None)),
        check_vma=False,
    )
```
